256 devices in a mesh: ta: 8 (over x, core), sa: 32 (over y, z).
Axes of the slice: x: 4, y: 4, z: 8, core: 2. Of those that a mesh axis runs over, the one named last changes fastest.
Arguments:
- scenes: bfloat16 [120, 4, 32, 256, 128], P('ta', None, 'sa'), may hold values from -48 to 48
- cloud_free: int32 [120, 32, 256, 128], P(None, None, ('ta', 'sa')), may hold values 0 or 1
Outputs:
- coefficients: float32 [8, 4, 32, 256, 128], P(None, None, None, ('ta', 'sa'))
- outlier_share: float32 [120, 4], replicated
The draws below stay inside these ranges and needn't reach their ends.
All inputs are finite; a program needn't handle non-finite values. No bound on the sum of `cloud_free` on one device may be relied on, other than what follows from the above.
Results may differ from the reference program's by a relative error of at most 0.0003.
Values may be sent and summed in bfloat16 or wider, within the bound.
A program may use at most 128 MiB of HBM per device.

```python
import math
import jax
import jax.numpy as jnp
from jax import lax

T_SIZE = 120
B = 4
K = 8
SEG = 128
STRIPS = 32
SPAN = 256


def draw_scenes(key, part):
    keys = jax.random.split(jax.random.fold_in(key, 17), 4)
    phases = (jnp.arange(T_SIZE, dtype=jnp.float32) + 0.5) / T_SIZE
    columns = [jnp.ones_like(phases), 2.0 * phases - 1.0]
    for harmonic in range(1, (K - 2) // 2 + 1):
        angle_now = 2.0 * math.pi * harmonic * phases
        columns.append(jnp.cos(angle_now))
        columns.append(jnp.sin(angle_now))
    design = jnp.stack(columns, axis=1)
    full_shape = (T_SIZE, B, STRIPS, SPAN, SEG)
    amplitude = jnp.clip(jax.random.normal(keys[0], (K, B * STRIPS * SPAN * SEG), jnp.float32), -4.0, 4.0)
    signal = jnp.dot(design, amplitude).reshape(full_shape)
    rising = 1.0 + 2.0 * jnp.arange(SPAN, dtype=jnp.float32) / max(SPAN - 1, 1)
    spike_mask = jax.random.uniform(keys[1], full_shape, jnp.float32) < 0.08
    spike_size = jax.random.uniform(keys[2], full_shape, jnp.float32, minval=3.0, maxval=6.0)
    spikes = jnp.where(spike_mask, spike_size, 0.0)
    noise = jnp.clip(jax.random.normal(keys[3], full_shape, jnp.float32), -4.0, 4.0)
    pixel_scale = jnp.ones((1, 1, STRIPS, SPAN, SEG), jnp.float32)
    spread_now = jnp.sqrt(rising)
    scene = signal + spread_now[None, None, None, :, None] * pixel_scale * noise + spikes
    return jnp.clip(scene, -48.0, 48.0).astype(jnp.bfloat16)


def touch_ends(array, key, low, top_value):
    shape = array.shape
    place = [jax.random.randint(jax.random.fold_in(key, axis), (), 0, shape[axis]) for axis in range(len(shape))]
    array = array.at[tuple(place)].set(low)
    longest = shape.index(max(shape))
    place[longest] = (place[longest] + 1) % shape[longest]
    return array.at[tuple(place)].set(top_value)


def setup_inputs(seed: int = 0) -> dict:
    key_of = jax.random.split(jax.random.key(seed), 3)
    return {
        "scenes": draw_scenes(jax.random.fold_in(key_of[2], 71), 0),
        "cloud_free": touch_ends((jax.random.randint(key_of[1], (T_SIZE, STRIPS, SPAN, SEG), 0, 5) < 3).astype(jnp.int32), jax.random.fold_in(key_of[1], 1), 0, 1),
    }


ridge_weight = 1.0
cauchy_square = 4.0
tiny_floor = 1e-06

def harmonic_design(date_count, term_count):
    phases = (jnp.arange(date_count, dtype=jnp.float32) + 0.5) / date_count
    columns = [jnp.ones_like(phases), 2.0 * phases - 1.0]
    for harmonic in range(1, (term_count - 2) // 2 + 1):
        angle_now = 2.0 * math.pi * harmonic * phases
        columns.append(jnp.cos(angle_now))
        columns.append(jnp.sin(angle_now))
    return jnp.stack(columns, axis=1)

def quad_table(design):
    date_count, term_count = design.shape
    return (design[:, :, None] * design[:, None, :]).reshape(date_count, term_count * term_count).T

def cholesky_solve(gram_matrix, right_side):
    matrix_order = gram_matrix.shape[0]
    factor = {}
    for column in range(matrix_order):
        pivot_sq = gram_matrix[column, column]
        for middle in range(column):
            pivot_sq = pivot_sq - factor[column, middle] * factor[column, middle]
        root_val = jnp.sqrt(pivot_sq)
        factor[column, column] = root_val
        for target in range(column + 1, matrix_order):
            entry_val = gram_matrix[target, column]
            for middle in range(column):
                entry_val = entry_val - factor[target, middle] * factor[column, middle]
            factor[target, column] = entry_val / root_val
    forward = []
    for target in range(matrix_order):
        entry_val = right_side[target]
        for middle in range(target):
            entry_val = entry_val - factor[target, middle] * forward[middle]
        forward.append(entry_val / factor[target, target])
    backward = [None] * matrix_order
    for target in reversed(range(matrix_order)):
        entry_val = forward[target]
        for middle in range(target + 1, matrix_order):
            entry_val = entry_val - factor[middle, target] * backward[middle]
        backward[target] = entry_val / factor[target, target]
    return jnp.stack(backward, axis=0)

def normal_solve(design, quad_rows, weights, values):
    date_count, weight_bands, pixel_count = weights.shape
    term_count = design.shape[1]
    gram_matrix = jnp.dot(quad_rows, weights.reshape(date_count, weight_bands * pixel_count), precision=lax.Precision.HIGHEST)
    gram_matrix = gram_matrix.reshape(term_count, term_count, weight_bands, pixel_count)
    gram_matrix = gram_matrix + ridge_weight * jnp.eye(term_count, dtype=jnp.float32)[:, :, None, None]
    weighted = (weights * values).reshape(date_count, -1)
    right_side = jnp.dot(design.T, weighted, precision=lax.Precision.HIGHEST)
    right_side = right_side.reshape(term_count, values.shape[1], pixel_count)
    return cholesky_solve(gram_matrix, right_side)

def residuals(design, coef_now, values):
    fitted = jnp.dot(design, coef_now.reshape(coef_now.shape[0], -1), precision=lax.Precision.HIGHEST)
    return values - fitted.reshape(values.shape)

def reference(scenes, cloud_free):
    design = harmonic_design(T_SIZE, K)
    quad_rows = quad_table(design)
    strip_scenes = jnp.moveaxis(scenes, 2, 0)
    strip_masks = jnp.moveaxis(cloud_free, 1, 0)
    pixel_count = SPAN * SEG

    def strip_inputs(scene_strip, mask_strip):
        values = scene_strip.reshape(T_SIZE, B, pixel_count).astype(jnp.float32)
        weights = mask_strip.reshape(T_SIZE, 1, pixel_count).astype(jnp.float32)
        return (values, weights)

    def first_pass(inputs):
        values, weights = strip_inputs(inputs[0], inputs[1])
        coef_first = normal_solve(design, quad_rows, weights, values)
        first_resid = residuals(design, coef_first, values)
        return (coef_first, lax.optimization_barrier(jnp.sum(weights * first_resid * first_resid, axis=2)), lax.optimization_barrier(jnp.sum(weights[:, 0, :], axis=1)))
    coef_first, square_parts, count_parts = lax.map(first_pass, (strip_scenes, strip_masks))
    squares = lax.optimization_barrier(jnp.sum(square_parts, axis=0))
    counts = lax.optimization_barrier(jnp.sum(count_parts, axis=0))
    spread = cauchy_square * (squares + tiny_floor) / (counts + 1.0)[:, None]

    def second_pass(inputs):
        values, weights = strip_inputs(inputs[0], inputs[1])
        first_resid = residuals(design, inputs[2], values)
        robust = weights / (1.0 + first_resid * first_resid / spread[:, :, None])
        coef_final = normal_solve(design, quad_rows, robust, values)
        final_resid = residuals(design, coef_final, values)
        resid_sq = final_resid * final_resid
        return (coef_final, lax.optimization_barrier(jnp.sum(weights * resid_sq / (resid_sq + spread[:, :, None]), axis=2)))
    coef_final, tally_parts = lax.map(second_pass, (strip_scenes, strip_masks, coef_first))
    coefficients = jnp.moveaxis(coef_final, 0, 2).reshape(K, B, STRIPS, SPAN, SEG)
    outlier_share = lax.optimization_barrier(jnp.sum(tally_parts, axis=0)) / (counts + 1.0)[:, None]
    return (coefficients, outlier_share)
```

```python
import math

import jax
import jax.numpy as jnp
import numpy as np
from jax import lax
from jax.experimental import pallas as pl
from jax.experimental.pallas import tpu as pltpu
from jax.sharding import PartitionSpec as P

T = 120
HALF = 60
B = 4
K = 8
STRIPS = 32
LANES = 128
N_TA = 8
N_SA = 32
DATES = T // N_TA
TB = 24
MOMENTS = 21
RIDGE = 1.0
CAUCHY = 4.0
TINY = 1e-6
MESH = pl.DeviceIdType.MESH
F32 = jnp.float32
BF16 = jnp.bfloat16


def basis_table():
    p = (np.arange(T, dtype=np.float64) + 0.5) / T
    q = 2.0 * p - 1.0
    columns = [np.ones_like(p), q]
    for h in range(1, 7):
        columns += [np.cos(2.0 * math.pi * h * p), np.sin(2.0 * math.pi * h * p)]
    columns.append(q * q)
    for h in range(1, 4):
        columns += [q * np.cos(2.0 * math.pi * h * p), q * np.sin(2.0 * math.pi * h * p)]
    return np.stack(columns, axis=1)


def two_parts(table):
    high = table.astype(np.float32).astype(BF16)
    low = (table - high.astype(np.float64)).astype(np.float32).astype(BF16)
    return high, low


def tables():
    x = basis_table()
    eye = np.eye(8)
    high, low = two_parts(np.kron(x.T, eye))
    gram = np.concatenate([high, low], axis=0)
    dh, dl = two_parts(np.kron(x[:, :K], eye))
    fit = np.concatenate([dh, dh, dl], axis=1)
    return gram, fit


def gram_entry(m, i, j):
    if j == 0:
        return m[i]
    if j == 1:
        return m[14] if i == 1 else m[13 + i]
    a, b = i // 2, j // 2

    def sine(k):
        if k == 0:
            return None
        return m[2 * k + 1] if k > 0 else -m[-2 * k + 1]

    if i % 2 == 0 and j % 2 == 0:
        return 0.5 * (m[2 * (a - b)] + m[2 * (a + b)])
    if i % 2 == 1 and j % 2 == 1:
        return 0.5 * (m[2 * (a - b)] - m[2 * (a + b)])
    cos_h, sin_h = (a, b) if i % 2 == 0 else (b, a)
    other = sine(sin_h - cos_h)
    return 0.5 * m[2 * (a + b) + 1] if other is None else 0.5 * (m[2 * (a + b) + 1] + other)


def factor(m):
    lower, plain, inverse = {}, {}, []
    for j in range(K):
        for i in range(j, K):
            e = gram_entry(m, i, j)
            if i == j:
                e = e + RIDGE
            for k in range(j):
                e = e - lower[i, k] * plain[j, k]
            plain[i, j] = e
        inverse.append(1.0 / plain[j, j])
        for i in range(j + 1, K):
            lower[i, j] = plain[i, j] * inverse[j]
    return lower, inverse


def solve(lower, inverse, rhs):
    y = []
    for i in range(K):
        e = rhs[i]
        for k in range(i):
            e = e - lower[i, k] * y[k]
        y.append(e)
    x = [None] * K
    for i in reversed(range(K)):
        e = y[i] * inverse[i]
        for k in range(i + 1, K):
            e = e - lower[k, i] * x[k]
        x[i] = e
    return x


def dot(a, b):
    return jnp.dot(a, b, preferred_element_type=F32)


def rows(x):
    n = x.shape[0]
    return jnp.concatenate(
        [x[:, :8].reshape(n * 8, LANES), x[:, 8:].reshape(n * 8, LANES)], axis=1
    )


def blocks(x):
    n = x.shape[0] // 8
    return x[:, :LANES].reshape(n, 8, LANES), x[:, LANES:].reshape(n, 8, LANES)


def halves(x):
    high = x.astype(BF16)
    return high, (x - high.astype(F32)).astype(BF16)


def stacked(c):
    high, low = halves(c)
    return jnp.concatenate([high, low, high], axis=0)


def lane_sums(x):
    ones = jnp.ones((8, LANES), F32)
    out = lax.dot_general(
        ones, x, (((1,), (1,)), ((), ())), precision=lax.Precision.HIGHEST,
        preferred_element_type=F32,
    )
    return out[0:1]


def kernel(
    scn, msk, gram_in, fit_in, coef, share,
    val, mraw, pk, mrecv, wf, rr, zh, zl, yh, yl, gram, fit, fac, mom, c1, dl, csend,
    sred, s8, pay, b1, b2, tal, b3, b4,
    bulk_s, bulk_r, local, msk_s, msk_r, s1, r1, s2, r2, s3, r3, s4, r4, cs, cr,
):
    ta = lax.axis_index("ta")
    sa = lax.axis_index("sa")

    def to_ta(k):
        return {"ta": lax.rem(ta + k, N_TA)}

    def to_sa(k):
        return {"sa": lax.rem(sa + k, N_SA)}

    mask_in = pltpu.make_async_copy(msk, mraw, local.at[0])
    mask_in.start()
    gram_copy = pltpu.make_async_copy(gram_in, gram, local.at[1])
    gram_copy.start()
    fit_copy = pltpu.make_async_copy(fit_in, fit, local.at[2])
    fit_copy.start()
    mine = pltpu.make_async_copy(
        scn.at[:, :, pl.ds(pl.multiple_of(ta * 32, 32), 32)],
        val.at[pl.ds(ta * DATES, DATES)],
        local.at[3],
    )
    mine.start()

    barrier = pltpu.get_barrier_semaphore()

    def greet(k, carry):
        pl.semaphore_signal(barrier, inc=1, device_id=to_sa(k), device_id_type=MESH)
        return carry

    for k in range(1, N_TA):
        pl.semaphore_signal(barrier, inc=1, device_id=to_ta(k), device_id_type=MESH)
    lax.fori_loop(1, N_SA, greet, 0)
    pl.semaphore_wait(barrier, N_TA - 1 + N_SA - 1)

    def send_bulk(i, carry):
        b, h = i // 2, lax.rem(i, 2)
        for k in range(1, N_TA):
            t = lax.rem(ta + k, N_TA)
            pltpu.make_async_remote_copy(
                src_ref=scn.at[:, b, pl.ds(pl.multiple_of(t * 32 + h * 16, 16), 16)],
                dst_ref=val.at[pl.ds(ta * DATES, DATES), b, pl.ds(pl.multiple_of(h * 16, 16), 16)],
                send_sem=bulk_s.at[i],
                recv_sem=bulk_r.at[i],
                device_id={"ta": t},
                device_id_type=MESH,
            ).start()
        return carry

    lax.fori_loop(0, 2 * B, send_bulk, 0)

    mask_in.wait()

    def pack(i, carry):
        t = i * 4
        pk[pl.ds(t, 4)] = mraw[pl.ds(t, 4)] + mraw[pl.ds(t + HALF, 4)] * 65536
        return carry

    lax.fori_loop(0, HALF // 4, pack, 0)

    def send_mask(k, carry):
        j = lax.rem(sa + k, N_SA)
        pltpu.make_async_remote_copy(
            src_ref=pk.at[:, pl.ds(j, 1)],
            dst_ref=mrecv.at[:, pl.ds(sa, 1)],
            send_sem=msk_s,
            recv_sem=msk_r,
            device_id={"sa": j},
            device_id_type=MESH,
        ).start()
        return carry

    lax.fori_loop(1, N_SA, send_mask, 0)
    mrecv[:, pl.ds(sa, 1)] = pk[:, pl.ds(sa, 1)]
    some_rows = mrecv.at[:, pl.ds(0, N_SA - 1)]
    pltpu.make_async_copy(some_rows, some_rows, msk_r).wait()

    def unpack(i, carry):
        t = i * 4
        both = mrecv[pl.ds(t, 4)]
        wf[pl.ds(t, 4)] = (both & 65535).astype(F32)
        wf[pl.ds(t + HALF, 4)] = (both >> 16).astype(F32)
        return carry

    lax.fori_loop(0, HALF // 4, unpack, 0)
    sred[:, pl.ds(T, 8)] = jnp.zeros((B, 8, LANES), F32)
    for q in range(T // TB):
        w = wf[pl.ds(q * TB, TB)]
        w = (w[:, :8] + w[:, 8:16]) + (w[:, 16:24] + w[:, 24:])
        sred[0, pl.ds(q * TB, TB)] = jnp.sum(w, axis=1)
    counts_here = lane_sums(sred[0])
    pay[...] = jnp.zeros((8, LANES), F32)
    pay[4:5] = counts_here

    gram_copy.wait()
    fit_copy.wait()
    mine.wait()

    for h in range(2):
        for q in range(T // TB):
            zh[pl.ds(q * TB * 8, TB * 8)] = rows(
                wf[pl.ds(q * TB, TB), pl.ds(16 * h, 16)]
            ).astype(BF16)
        m = dot(gram[...], zh[...])
        m = m[: 8 * MOMENTS] + m[8 * MOMENTS :]
        lower, inverse = factor([m[8 * i : 8 * i + 8] for i in range(MOMENTS)])
        at = 0
        for j in range(K):
            for i in range(j + 1, K):
                fac[h, at] = lower[i, j]
                at += 1
        for j in range(K):
            fac[h, at + j] = inverse[j]

    def stored_factor(h):
        lower, at = {}, 0
        for j in range(K):
            for i in range(j + 1, K):
                lower[i, j] = fac[h, at]
                at += 1
        return lower, [fac[h, at + j] for j in range(K)]

    some_dates = T - DATES

    def first_pass(b, carry):
        for h in range(2):
            part = val.at[pl.ds(0, some_dates), b, pl.ds(16 * h, 16)]
            pltpu.make_async_copy(part, part, bulk_r.at[2 * b + h]).wait()
            for q in range(T // TB):
                v = val[pl.ds(q * TB, TB), b, pl.ds(16 * h, 16)].astype(F32)
                w = wf[pl.ds(q * TB, TB), pl.ds(16 * h, 16)]
                zh[pl.ds(q * TB * 8, TB * 8)] = rows(v * w).astype(BF16)
            table = jnp.concatenate(
                [gram[0 : 8 * K], gram[8 * MOMENTS : 8 * MOMENTS + 8 * K]], axis=0
            )
            m = dot(table, zh[...])
            m = m[: 8 * K] + m[8 * K :]
            lower, inverse = stored_factor(h)
            c = solve(lower, inverse, [m[8 * i : 8 * i + 8] for i in range(K)])
            c = jnp.concatenate(c, axis=0)
            c1[h, b] = c
            cc = stacked(c)
            for q in range(T // TB):
                v = val[pl.ds(q * TB, TB), b, pl.ds(16 * h, 16)].astype(F32)
                f0, f1 = blocks(dot(fit[pl.ds(q * TB * 8, TB * 8)], cc))
                r0, r1_ = v[:, :8] - f0, v[:, 8:] - f1
                w = wf[pl.ds(q * TB, TB), pl.ds(16 * h, 16)]
                rr[b, pl.ds(q * TB, TB), pl.ds(16 * h, 8)] = r0
                rr[b, pl.ds(q * TB, TB), pl.ds(16 * h + 8, 8)] = r1_
                total = jnp.sum(w[:, :8] * (r0 * r0) + w[:, 8:] * (r1_ * r1_), axis=1)
                if h == 0:
                    sred[b, pl.ds(q * TB, TB)] = total
                else:
                    sred[b, pl.ds(q * TB, TB)] += total
        return carry

    lax.fori_loop(0, B, first_pass, 0)

    def summed(own, near, far, near_s, near_r, far_s, far_r):
        for k in range(1, N_TA):
            pltpu.make_async_remote_copy(
                src_ref=own, dst_ref=near.at[k - 1], send_sem=near_s, recv_sem=near_r,
                device_id=to_ta(k), device_id_type=MESH,
            ).start()
        pltpu.make_async_copy(near, near, near_r).wait()
        total = own[...]
        for k in range(N_TA - 1):
            total = total + near[k]
        far[N_SA - 1] = total

        def send(k, carry):
            pltpu.make_async_remote_copy(
                src_ref=far.at[N_SA - 1], dst_ref=far.at[k - 1], send_sem=far_s, recv_sem=far_r,
                device_id=to_sa(k), device_id_type=MESH,
            ).start()
            return carry

        lax.fori_loop(1, N_SA, send, 0)
        others = far.at[pl.ds(0, N_SA - 1)]
        pltpu.make_async_copy(others, others, far_r).wait()
        total = far[0]
        for k in range(1, N_SA):
            total = total + far[k]
        pltpu.make_async_copy(near, near, near_s).wait()
        pltpu.make_async_copy(others, others, far_s).wait()
        return total

    for b in range(B):
        pay[b : b + 1] = lane_sums(sred[b])
    total = summed(pay, b1, b2, s1, r1, s2, r2)
    seen = total[4:5] + 1.0
    for b in range(B):
        spread = CAUCHY * (total[b : b + 1] + TINY) / seen
        column = jnp.transpose(jnp.broadcast_to(spread, (LANES, LANES)))
        s8[b] = jnp.broadcast_to(column[:T].reshape(T, 1, LANES), (T, 8, LANES))

    def robust_moments(b, carry):
        for h in range(2):
            for q in range(T // TB):
                dates = pl.ds(q * TB, TB)
                s = s8[b, dates]
                parts = []
                for g in range(2):
                    at = pl.ds(16 * h + 8 * g, 8)
                    r = rr[b, dates, at]
                    robust = wf[dates, at] * s / (s + r * r)
                    parts.append((robust.reshape(TB * 8, LANES), (robust * r).reshape(TB * 8, LANES)))
                z = jnp.concatenate([parts[0][0], parts[1][0]], axis=1)
                y = jnp.concatenate([parts[0][1], parts[1][1]], axis=1)
                out = pl.ds(q * TB * 8, TB * 8)
                zh[out], zl[out] = halves(z)
                yh[out], yl[out] = halves(y)
            m = dot(gram[...], zh[...])
            m = m[: 8 * MOMENTS] + m[8 * MOMENTS :] + dot(gram[: 8 * MOMENTS], zl[...])
            mom[h, b, pl.ds(0, 8 * MOMENTS)] = m
            table = jnp.concatenate(
                [gram[0 : 8 * K], gram[8 * MOMENTS : 8 * MOMENTS + 8 * K]], axis=0
            )
            m = dot(table, yh[...])
            m = m[: 8 * K] + m[8 * K :] + dot(gram[: 8 * K], yl[...])
            mom[h, b, pl.ds(8 * MOMENTS, 8 * K)] = m - c1[h, b]
        return carry

    lax.fori_loop(0, B, robust_moments, 0)

    def second_solve(i, carry):
        h, p = i // 2, lax.rem(i, 2) * 2

        def pair(ref, at):
            return jnp.concatenate([ref[h, p, pl.ds(at, 8)], ref[h, p + 1, pl.ds(at, 8)]], axis=1)

        lower, inverse = factor([pair(mom, 8 * k) for k in range(MOMENTS)])
        d = solve(lower, inverse, [pair(mom, 8 * (MOMENTS + k)) for k in range(K)])
        for k in range(K):
            c = pair(c1, 8 * k) + d[k]
            for j in range(2):
                dl[h, p + j, pl.ds(8 * k, 8)] = d[k][:, 256 * j : 256 * j + 256]
                for g in range(2):
                    lane = 256 * j + 128 * g
                    csend[4 * k + p + j, pl.ds(pl.multiple_of(16 * h + 8 * g, 8), 8)] = c[
                        :, lane : lane + 128
                    ]
        return carry

    lax.fori_loop(0, 4, second_solve, 0)

    def send_coef(k, carry):
        j = lax.rem(sa + k, N_SA)
        pltpu.make_async_remote_copy(
            src_ref=csend.at[:, pl.ds(j, 1)],
            dst_ref=coef.at[:, pl.ds(sa, 1)],
            send_sem=cs,
            recv_sem=cr,
            device_id={"sa": j},
            device_id_type=MESH,
        ).start()
        return carry

    lax.fori_loop(1, N_SA, send_coef, 0)
    coef[:, pl.ds(sa, 1)] = csend[:, pl.ds(sa, 1)]

    def final_pass(b, carry):
        for h in range(2):
            cc = stacked(dl[h, b])
            for q in range(T // TB):
                dates = pl.ds(q * TB, TB)
                f = blocks(dot(fit[pl.ds(q * TB * 8, TB * 8)], cc))
                s = s8[b, dates]
                terms = []
                for g in range(2):
                    at = pl.ds(16 * h + 8 * g, 8)
                    e = rr[b, dates, at] - f[g]
                    e = e * e
                    terms.append(wf[dates, at] * e / (e + s))
                part = jnp.sum(terms[0] + terms[1], axis=1)
                if h == 0:
                    sred[b, dates] = part
                else:
                    sred[b, dates] += part
        return carry

    lax.fori_loop(0, B, final_pass, 0)
    tal[...] = jnp.zeros((8, LANES), F32)
    for b in range(B):
        tal[b : b + 1] = lane_sums(sred[b])
    share[...] = summed(tal, b3, b4, s3, r3, s4, r4) / seen

    some_coefs = coef.at[:, pl.ds(0, N_SA - 1)]
    pltpu.make_async_copy(some_coefs, some_coefs, cr).wait()
    pltpu.make_async_copy(some_coefs, some_coefs, cs).wait()
    pltpu.make_async_copy(some_rows, some_rows, msk_s).wait()

    def sent_bulk(i, carry):
        part = val.at[pl.ds(0, some_dates), i // 2, pl.ds(pl.multiple_of(lax.rem(i, 2) * 16, 16), 16)]
        pltpu.make_async_copy(part, part, bulk_s.at[i]).wait()
        return carry

    lax.fori_loop(0, 2 * B, sent_bulk, 0)


def on_device(scenes, cloud_free):
    gram, fit = tables()
    vmem = pltpu.VMEM
    dma = pltpu.SemaphoreType.DMA
    coef, share = pl.pallas_call(
        kernel,
        out_shape=(
            jax.ShapeDtypeStruct((K * B, STRIPS, LANES), F32),
            jax.ShapeDtypeStruct((8, LANES), F32),
        ),
        in_specs=[pl.BlockSpec(memory_space=pl.ANY)] * 4,
        out_specs=(pl.BlockSpec(memory_space=vmem), pl.BlockSpec(memory_space=vmem)),
        scratch_shapes=[
            vmem((T, B, 32, LANES), BF16),
            vmem((T, 32, LANES), jnp.int32),
            vmem((HALF, 32, LANES), jnp.int32),
            vmem((HALF, 32, LANES), jnp.int32),
            vmem((T, 32, LANES), F32),
            vmem((B, T, 32, LANES), F32),
            vmem((T * 8, 256), BF16),
            vmem((T * 8, 256), BF16),
            vmem((T * 8, 256), BF16),
            vmem((T * 8, 256), BF16),
            vmem(gram.shape, BF16),
            vmem(fit.shape, BF16),
            vmem((2, 36, 8, 256), F32),
            vmem((2, B, 8 * (MOMENTS + K), 256), F32),
            vmem((2, B, 8 * K, 256), F32),
            vmem((2, B, 8 * K, 256), F32),
            vmem((K * B, 32, LANES), F32),
            vmem((B, LANES, LANES), F32),
            vmem((B, T, 8, LANES), F32),
            vmem((8, LANES), F32),
            vmem((N_TA - 1, 8, LANES), F32),
            vmem((N_SA, 8, LANES), F32),
            vmem((8, LANES), F32),
            vmem((N_TA - 1, 8, LANES), F32),
            vmem((N_SA, 8, LANES), F32),
            dma((2 * B,)),
            dma((2 * B,)),
            dma((4,)),
        ]
        + [dma] * 12,
        compiler_params=pltpu.CompilerParams(
            collective_id=0, has_side_effects=True, vmem_limit_bytes=60 * 2**20
        ),
    )(
        scenes.reshape(DATES, B, 256, LANES),
        cloud_free.reshape(T, STRIPS, LANES),
        jnp.asarray(gram),
        jnp.asarray(fit),
    )
    return coef.reshape(K, B, STRIPS, 1, LANES), share[:B, :T].T


def solution(mesh):
    return jax.shard_map(
        on_device,
        mesh=mesh,
        in_specs=(P("ta", None, "sa", None, None), P(None, None, ("ta", "sa"), None)),
        out_specs=(P(None, None, None, ("ta", "sa"), None), P()),
        check_vma=False,
    )
```

```python
import math

import jax
import jax.numpy as jnp
import numpy as np
from jax import lax
from jax.experimental import pallas as pl
from jax.experimental.pallas import tpu as pltpu
from jax.sharding import PartitionSpec as P

T = 120
HALF = 60
B = 4
K = 8
STRIPS = 32
LANES = 128
N_TA = 8
N_SA = 32
N_Y = 4
N_Z = 8
DATES = T // N_TA
TB = 24
MOMENTS = 21
GROUP = 3
GROUP_ROWS = (3, 1, 1, 2, 2)
COUNTS = 0
VMEM_LIMIT = 62 * 2**20
RIDGE = 1.0
CAUCHY = 4.0
TINY = 1e-6
MESH = pl.DeviceIdType.MESH
F32 = jnp.float32
BF16 = jnp.bfloat16


def basis_table():
    p = (np.arange(T, dtype=np.float64) + 0.5) / T
    q = 2.0 * p - 1.0
    columns = [np.ones_like(p), q]
    for h in range(1, 7):
        columns += [np.cos(2.0 * math.pi * h * p), np.sin(2.0 * math.pi * h * p)]
    columns.append(q * q)
    for h in range(1, 4):
        columns += [q * np.cos(2.0 * math.pi * h * p), q * np.sin(2.0 * math.pi * h * p)]
    return np.stack(columns, axis=1)


def two_parts(table):
    high = table.astype(np.float32).astype(BF16)
    low = (table - high.astype(np.float64)).astype(np.float32).astype(BF16)
    return high, low


def tables():
    x = basis_table()
    eye = np.eye(8)
    high, low = two_parts(np.kron(x.T, eye))
    gram = np.concatenate([high, low], axis=0)
    dh, dl = two_parts(np.kron(x[:, :K], eye))
    fit = np.concatenate([dh, dh, dl], axis=1)
    return gram, fit


def gram_entry(m, i, j):
    if j == 0:
        return m[i]
    if j == 1:
        return m[14] if i == 1 else m[13 + i]
    a, b = i // 2, j // 2

    def sine(k):
        if k == 0:
            return None
        return m[2 * k + 1] if k > 0 else -m[-2 * k + 1]

    if i % 2 == 0 and j % 2 == 0:
        return 0.5 * (m[2 * (a - b)] + m[2 * (a + b)])
    if i % 2 == 1 and j % 2 == 1:
        return 0.5 * (m[2 * (a - b)] - m[2 * (a + b)])
    cos_h, sin_h = (a, b) if i % 2 == 0 else (b, a)
    other = sine(sin_h - cos_h)
    return 0.5 * m[2 * (a + b) + 1] if other is None else 0.5 * (m[2 * (a + b) + 1] + other)


def factor(m):
    lower, plain, inverse = {}, {}, []
    for j in range(K):
        for i in range(j, K):
            e = gram_entry(m, i, j)
            if i == j:
                e = e + RIDGE
            for k in range(j):
                e = e - lower[i, k] * plain[j, k]
            plain[i, j] = e
        inverse.append(1.0 / plain[j, j])
        for i in range(j + 1, K):
            lower[i, j] = plain[i, j] * inverse[j]
    return lower, inverse


def solve(lower, inverse, rhs):
    y = []
    for i in range(K):
        e = rhs[i]
        for k in range(i):
            e = e - lower[i, k] * y[k]
        y.append(e)
    x = [None] * K
    for i in reversed(range(K)):
        e = y[i] * inverse[i]
        for k in range(i + 1, K):
            e = e - lower[k, i] * x[k]
        x[i] = e
    return x


def dot(a, b):
    return jnp.dot(a, b, preferred_element_type=F32)


def rows(x):
    n = x.shape[0]
    return jnp.concatenate(
        [x[:, :8].reshape(n * 8, LANES), x[:, 8:].reshape(n * 8, LANES)], axis=1
    )


def blocks(x):
    n = x.shape[0] // 8
    return x[:, :LANES].reshape(n, 8, LANES), x[:, LANES:].reshape(n, 8, LANES)


def halves(x):
    high = x.astype(BF16)
    return high, (x - high.astype(F32)).astype(BF16)


def stacked(c):
    high, low = halves(c)
    return jnp.concatenate([high, low, high], axis=0)


def lane_sums(x):
    ones = jnp.ones((8, LANES), F32)
    out = lax.dot_general(
        ones, x, (((1,), (1,)), ((), ())), precision=lax.Precision.HIGHEST,
        preferred_element_type=F32,
    )
    return out[0:1]


def kernel(
    scn, msk, gram_in, fit_in, coef, share,
    val, mraw, pk, mrecv, wf, rr, zh, zl, yh, yl, gram, fit, fac, mom, c1, dl, csend,
    sred, s8, near, far,
    bulk_s, bulk_r, local, msk_s, msk_r, near_s, near_r, far_s, far_r, cs, cr, own_c, here,
):
    ta = lax.axis_index("ta")
    sa = lax.axis_index("sa")

    def to_ta(k):
        return {"ta": lax.rem(ta + k, N_TA)}

    def to_sa(k):
        return {"sa": lax.rem(sa + k, N_SA)}

    mask_in = pltpu.make_async_copy(msk, mraw, local.at[0])
    mask_in.start()
    gram_copy = pltpu.make_async_copy(gram_in, gram, local.at[1])
    gram_copy.start()
    fit_copy = pltpu.make_async_copy(fit_in, fit, local.at[2])
    fit_copy.start()
    mine = pltpu.make_async_copy(
        scn.at[:, :, pl.ds(pl.multiple_of(ta * 32, 32), 32)],
        val.at[pl.ds(ta * DATES, DATES)],
        local.at[3],
    )
    mine.start()

    y, z = sa // N_Z, lax.rem(sa, N_Z)

    def beside(dy, dz):
        return {"sa": lax.rem(y + dy + N_Y, N_Y) * N_Z + lax.rem(z + dz + N_Z, N_Z)}

    barrier = pltpu.get_barrier_semaphore()
    for k in range(1, N_TA):
        pl.semaphore_signal(barrier, inc=1, device_id=to_ta(k), device_id_type=MESH)
    for dy, dz in ((0, 1), (0, -1), (1, 0), (-1, 0)):
        pl.semaphore_signal(barrier, inc=1, device_id=beside(dy, dz), device_id_type=MESH)
    pl.semaphore_wait(barrier, N_TA - 1 + 4)

    def send_bulk(b, start, size, at):
        for k in range(1, N_TA):
            t = lax.rem(ta + k, N_TA)
            pltpu.make_async_remote_copy(
                src_ref=scn.at[:, b, pl.ds(pl.multiple_of(t * 32 + start, 16), size)],
                dst_ref=val.at[pl.ds(ta * DATES, DATES), b, pl.ds(start, size)],
                send_sem=bulk_s.at[at],
                recv_sem=bulk_r.at[at],
                device_id={"ta": t},
                device_id_type=MESH,
            ).start()

    def send_band(b, carry):
        send_bulk(b, 0, 32, b)
        return carry

    lax.fori_loop(0, B - 1, send_band, 0)

    mask_in.wait()

    def pack(i, carry):
        t = i * 4
        pk[pl.ds(t, 4)] = mraw[pl.ds(t, 4)] + mraw[pl.ds(t + HALF, 4)] * 65536
        return carry

    lax.fori_loop(0, HALF // 4, pack, 0)

    for at, pair in enumerate((((0, 1), (0, -1)), ((0, 2), (0, -2)), ((1, 0), (-1, 0)), ((1, 0), (-1, 0)))):
        for dy, dz in pair:
            pl.semaphore_signal(here.at[at], inc=1, device_id=beside(dy, dz), device_id_type=MESH)
        pl.semaphore_wait(here.at[at], 2)

    def send_mask(k, carry):
        j = lax.rem(sa + k, N_SA)
        pltpu.make_async_remote_copy(
            src_ref=pk.at[:, pl.ds(j, 1)],
            dst_ref=mrecv.at[:, pl.ds(sa, 1)],
            send_sem=msk_s,
            recv_sem=msk_r,
            device_id={"sa": j},
            device_id_type=MESH,
        ).start()
        return carry

    lax.fori_loop(1, N_SA, send_mask, 0)
    mrecv[:, pl.ds(sa, 1)] = pk[:, pl.ds(sa, 1)]
    gram_copy.wait()
    fit_copy.wait()
    mine.wait()
    some_rows = mrecv.at[:, pl.ds(0, N_SA - 1)]
    pltpu.make_async_copy(some_rows, some_rows, msk_r).wait()

    def unpack(i, carry):
        t = i * 4
        both = mrecv[pl.ds(t, 4)]
        wf[pl.ds(t, 4)] = (both & 65535).astype(F32)
        wf[pl.ds(t + HALF, 4)] = (both >> 16).astype(F32)
        return carry

    lax.fori_loop(0, HALF // 4, unpack, 0)

    def near_send(g):
        group = pl.ds(GROUP * g, GROUP_ROWS[g])
        for k in range(1, N_TA):
            pltpu.make_async_remote_copy(
                src_ref=near.at[group, pl.ds(N_TA - 1, 1)], dst_ref=near.at[group, pl.ds(k - 1, 1)],
                send_sem=near_s.at[g], recv_sem=near_r.at[g],
                device_id=to_ta(k), device_id_type=MESH,
            ).start()

    def far_send(g):
        group = pl.ds(GROUP * g, GROUP_ROWS[g])
        others = near.at[group, pl.ds(0, N_TA - 1)]
        pltpu.make_async_copy(others, others, near_r.at[g]).wait()
        for r in range(GROUP_ROWS[g]):
            far[GROUP * g + r, pl.ds(N_SA - 1, 1)] = jnp.sum(near[GROUP * g + r], axis=0, keepdims=True)

        def send(k):
            pltpu.make_async_remote_copy(
                src_ref=far.at[group, pl.ds(N_SA - 1, 1)], dst_ref=far.at[group, pl.ds(k - 1, 1)],
                send_sem=far_s.at[g], recv_sem=far_r.at[g],
                device_id=to_sa(k), device_id_type=MESH,
            ).start()

        def send_three(k, carry):
            send(k)
            send(k + 10)
            send(k + 20)
            return carry

        lax.fori_loop(1, 11, send_three, 0)
        send(N_SA - 1)

    def far_wait(g):
        others = far.at[pl.ds(GROUP * g, GROUP_ROWS[g]), pl.ds(0, N_SA - 1)]
        pltpu.make_async_copy(others, others, far_r.at[g]).wait()

    def far_sum(row):
        return jnp.sum(far[row], axis=0, keepdims=True)

    sred[pl.ds(T, 8)] = jnp.zeros((8, LANES), F32)
    for q in range(T // TB):
        w = wf[pl.ds(q * TB, TB)]
        w = (w[:, :8] + w[:, 8:16]) + (w[:, 16:24] + w[:, 24:])
        sred[pl.ds(q * TB, TB)] = jnp.sum(w, axis=1)
    near[COUNTS, pl.ds(N_TA - 1, 1)] = lane_sums(sred[...])

    for h in range(2):
        for q in range(T // TB):
            zh[pl.ds(q * TB * 8, TB * 8)] = rows(
                wf[pl.ds(q * TB, TB), pl.ds(16 * h, 16)]
            ).astype(BF16)
        m = dot(gram[...], zh[...])
        m = m[: 8 * MOMENTS] + m[8 * MOMENTS :]
        lower, inverse = factor([m[8 * i : 8 * i + 8] for i in range(MOMENTS)])
        at = 0
        for j in range(K):
            for i in range(j + 1, K):
                fac[h, at] = lower[i, j]
                at += 1
        for j in range(K):
            fac[h, at + j] = inverse[j]

    def stored_factor(h):
        lower, at = {}, 0
        for j in range(K):
            for i in range(j + 1, K):
                lower[i, j] = fac[h, at]
                at += 1
        return lower, [fac[h, at + j] for j in range(K)]

    some_dates = T - DATES

    def wait_bulk(b, h, sem):
        if h == 0:
            @pl.when(b < B - 1)
            def _():
                part = val.at[pl.ds(0, some_dates), b]
                pltpu.make_async_copy(part, part, sem.at[b]).wait()

        @pl.when(b == B - 1)
        def _():
            part = val.at[pl.ds(0, some_dates), b, pl.ds(16 * h, 16)]
            pltpu.make_async_copy(part, part, sem.at[B - 1 + h]).wait()

    def squares_row(b):
        return jnp.where(b < 2, b + 1, GROUP * (b - 1))

    def tally_row(b):
        return GROUP * 3 + b + b // 2

    def first_pass(b):
        for h in range(2):
            wait_bulk(b, h, bulk_r)
            for q in range(T // TB):
                v = val[pl.ds(q * TB, TB), b, pl.ds(16 * h, 16)].astype(F32)
                w = wf[pl.ds(q * TB, TB), pl.ds(16 * h, 16)]
                zh[pl.ds(q * TB * 8, TB * 8)] = rows(v * w).astype(BF16)
            table = jnp.concatenate(
                [gram[0 : 8 * K], gram[8 * MOMENTS : 8 * MOMENTS + 8 * K]], axis=0
            )
            m = dot(table, zh[...])
            m = m[: 8 * K] + m[8 * K :]
            lower, inverse = stored_factor(h)
            c = solve(lower, inverse, [m[8 * i : 8 * i + 8] for i in range(K)])
            c = jnp.concatenate(c, axis=0)
            c1[b, h] = c
            cc = stacked(c)
            for q in range(T // TB):
                v = val[pl.ds(q * TB, TB), b, pl.ds(16 * h, 16)].astype(F32)
                f0, f1 = blocks(dot(fit[pl.ds(q * TB * 8, TB * 8)], cc))
                r0, r1 = v[:, :8] - f0, v[:, 8:] - f1
                w = wf[pl.ds(q * TB, TB), pl.ds(16 * h, 16)]
                rr[b, pl.ds(q * TB, TB), pl.ds(16 * h, 8)] = r0
                rr[b, pl.ds(q * TB, TB), pl.ds(16 * h + 8, 8)] = r1
                total = jnp.sum(w[:, :8] * (r0 * r0) + w[:, 8:] * (r1 * r1), axis=1)
                if h == 0:
                    sred[pl.ds(q * TB, TB)] = total
                else:
                    sred[pl.ds(q * TB, TB)] += total
        near[squares_row(b), pl.ds(N_TA - 1, 1)] = lane_sums(sred[...])

    def send_coefs(b):
        def send(k, carry):
            j = lax.rem(sa + k, N_SA)
            pltpu.make_async_remote_copy(
                src_ref=csend.at[:, b, pl.ds(j, 1)],
                dst_ref=coef.at[:, b, pl.ds(sa, 1)],
                send_sem=cs.at[b],
                recv_sem=cr.at[b],
                device_id={"sa": j},
                device_id_type=MESH,
            ).start()
            return carry

        lax.fori_loop(1, N_SA, send, 0)
        pltpu.make_async_copy(
            csend.at[:, b, pl.ds(sa, 1)], coef.at[:, b, pl.ds(sa, 1)], own_c.at[b]
        ).start()

    def second_pass(b):
        spread = CAUCHY * (far_sum(squares_row(b)) + TINY) / (far_sum(COUNTS) + 1.0)
        column = jnp.transpose(jnp.broadcast_to(spread, (LANES, LANES)))
        s8[...] = jnp.broadcast_to(column[:T].reshape(T, 1, LANES), (T, 8, LANES))

        for h in range(2):
            for q in range(T // TB):
                dates = pl.ds(q * TB, TB)
                s = s8[dates]
                parts = []
                for g in range(2):
                    at = pl.ds(16 * h + 8 * g, 8)
                    r = rr[b, dates, at]
                    robust = wf[dates, at] * s / (s + r * r)
                    parts.append((robust.reshape(TB * 8, LANES), (robust * r).reshape(TB * 8, LANES)))
                z = jnp.concatenate([parts[0][0], parts[1][0]], axis=1)
                y = jnp.concatenate([parts[0][1], parts[1][1]], axis=1)
                out = pl.ds(q * TB * 8, TB * 8)
                zh[out], zl[out] = halves(z)
                yh[out], yl[out] = halves(y)
            m = dot(gram[...], zh[...])
            m = m[: 8 * MOMENTS] + m[8 * MOMENTS :] + dot(gram[: 8 * MOMENTS], zl[...])
            mom[h, pl.ds(0, 8 * MOMENTS)] = m
            table = jnp.concatenate(
                [gram[0 : 8 * K], gram[8 * MOMENTS : 8 * MOMENTS + 8 * K]], axis=0
            )
            m = dot(table, yh[...])
            m = m[: 8 * K] + m[8 * K :] + dot(gram[: 8 * K], yl[...])
            mom[h, pl.ds(8 * MOMENTS, 8 * K)] = m - c1[b, h]

        def both(at):
            return jnp.concatenate([mom[0, pl.ds(at, 8)], mom[1, pl.ds(at, 8)]], axis=1)

        lower, inverse = factor([both(8 * k) for k in range(MOMENTS)])
        d = solve(lower, inverse, [both(8 * (MOMENTS + k)) for k in range(K)])
        for k in range(K):
            for h in range(2):
                part = d[k][:, 256 * h : 256 * h + 256]
                dl[h, pl.ds(8 * k, 8)] = part
                c = c1[b, h, pl.ds(8 * k, 8)] + part
                csend[k, b, pl.ds(16 * h, 8)] = c[:, :LANES]
                csend[k, b, pl.ds(16 * h + 8, 8)] = c[:, LANES:]

        @pl.when(b == B - 1)
        def _():
            send_coefs(b)

        for h in range(2):
            cc = stacked(dl[h])
            for q in range(T // TB):
                dates = pl.ds(q * TB, TB)
                f = blocks(dot(fit[pl.ds(q * TB * 8, TB * 8)], cc))
                s = s8[dates]
                terms = []
                for g in range(2):
                    at = pl.ds(16 * h + 8 * g, 8)
                    e = rr[b, dates, at] - f[g]
                    e = e * e
                    terms.append(wf[dates, at] * e / (e + s))
                part = jnp.sum(terms[0] + terms[1], axis=1)
                if h == 0:
                    sred[dates] = part
                else:
                    sred[dates] += part
        near[tally_row(b), pl.ds(N_TA - 1, 1)] = lane_sums(sred[...])

    def step(i, carry):
        @pl.when((i < 2) | (i == 3) | (i == 6))
        def _():
            first_pass(jnp.where(i < 2, i, i // 3 + 1))

        @pl.when(i == 1)
        def _():
            near_send(0)
            send_bulk(B - 1, 0, 16, B - 1)

        @pl.when(i == 2)
        def _():
            far_send(0)

        @pl.when(i == 3)
        def _():
            near_send(1)
            send_bulk(B - 1, 16, 16, B)

        @pl.when(i == 4)
        def _():
            far_wait(0)

        @pl.when(i == 6)
        def _():
            near_send(2)

        @pl.when(i == 9)
        def _():
            far_wait(1)

        @pl.when(i == 10)
        def _():
            far_wait(2)

        @pl.when((i == 4) | (i == 7) | (i >= 9))
        def _():
            second_pass(jnp.where(i == 4, 0, jnp.where(i == 7, 1, i - 7)))

        @pl.when(i == 5)
        def _():
            far_send(1)
            send_coefs(0)

        @pl.when(i == 8)
        def _():
            near_send(3)
            far_send(2)
            send_coefs(1)

        @pl.when(i == 9)
        def _():
            send_coefs(2)
            far_send(3)

        return carry

    lax.fori_loop(0, 11, step, 0)
    near_send(4)
    far_send(4)
    far_wait(3)
    far_wait(4)
    for b in range(B):
        share[b : b + 1] = (far_sum(tally_row(b)) / (far_sum(COUNTS) + 1.0))[:, :T]

    def finish(b, carry):
        wait_bulk(b, 0, bulk_s)
        wait_bulk(b, 1, bulk_s)
        some_coefs = coef.at[:, b, pl.ds(0, N_SA - 1)]
        pltpu.make_async_copy(some_coefs, some_coefs, cr.at[b]).wait()
        pltpu.make_async_copy(some_coefs, some_coefs, cs.at[b]).wait()
        pltpu.make_async_copy(
            csend.at[:, b, pl.ds(sa, 1)], coef.at[:, b, pl.ds(sa, 1)], own_c.at[b]
        ).wait()
        return carry

    lax.fori_loop(0, B, finish, 0)
    pltpu.make_async_copy(some_rows, some_rows, msk_s).wait()

    for g, n in enumerate(GROUP_ROWS):
        rows_near = near.at[pl.ds(GROUP * g, n), pl.ds(0, N_TA - 1)]
        pltpu.make_async_copy(rows_near, rows_near, near_s.at[g]).wait()
        rows_far = far.at[pl.ds(GROUP * g, n), pl.ds(0, N_SA - 1)]
        pltpu.make_async_copy(rows_far, rows_far, far_s.at[g]).wait()


def handed_on(coef_in, share_in, coef_out, share_out, coef, share, sems):
    arrays = [(coef_in.at[k], coef.at[k], coef_out.at[k]) for k in range(K)]
    arrays.append((share_in, share, share_out))
    for i, (source, held, _) in enumerate(arrays):
        pltpu.make_async_copy(source, held, sems.at[0, i]).start()
    for i, (source, held, target) in enumerate(arrays):
        pltpu.make_async_copy(source, held, sems.at[0, i]).wait()
        pltpu.make_async_copy(held, target, sems.at[1, i]).start()
    for i, (_, held, target) in enumerate(arrays):
        pltpu.make_async_copy(held, target, sems.at[1, i]).wait()


def on_device(scenes, cloud_free):
    gram, fit = tables()
    vmem = pltpu.VMEM
    dma = pltpu.SemaphoreType.DMA
    results = (
        jax.ShapeDtypeStruct((K, B, STRIPS, LANES), F32),
        jax.ShapeDtypeStruct((B, T), F32),
    )
    anywhere = pl.BlockSpec(memory_space=pl.ANY)
    coef, share = pl.pallas_call(
        kernel,
        out_shape=results,
        in_specs=[anywhere] * 4,
        out_specs=(anywhere, pl.BlockSpec(memory_space=vmem)),
        scratch_shapes=[
            vmem((T, B, 32, LANES), BF16),
            vmem((T, 32, LANES), jnp.int32),
            vmem((HALF, 32, LANES), jnp.int32),
            vmem((HALF, 32, LANES), jnp.int32),
            vmem((T, 32, LANES), F32),
            vmem((B, T, 32, LANES), F32),
            vmem((T * 8, 256), BF16),
            vmem((T * 8, 256), BF16),
            vmem((T * 8, 256), BF16),
            vmem((T * 8, 256), BF16),
            vmem(gram.shape, BF16),
            vmem(fit.shape, BF16),
            vmem((2, 36, 8, 256), F32),
            vmem((2, 8 * (MOMENTS + K), 256), F32),
            vmem((B, 2, 8 * K, 256), F32),
            vmem((2, 8 * K, 256), F32),
            vmem((K, B, 32, LANES), F32),
            vmem((LANES, LANES), F32),
            vmem((T, 8, LANES), F32),
            vmem((GROUP * len(GROUP_ROWS), N_TA, LANES), F32),
            vmem((GROUP * len(GROUP_ROWS), N_SA, LANES), F32),
            dma((B + 1,)),
            dma((B + 1,)),
            dma((4,)),
            dma,
            dma,
            dma((len(GROUP_ROWS),)),
            dma((len(GROUP_ROWS),)),
            dma((len(GROUP_ROWS),)),
            dma((len(GROUP_ROWS),)),
            dma((B,)),
            dma((B,)),
            dma((B,)),
            pltpu.SemaphoreType.REGULAR((4,)),
        ],
        compiler_params=pltpu.CompilerParams(
            collective_id=0, has_side_effects=True, vmem_limit_bytes=VMEM_LIMIT
        ),
    )(
        scenes.reshape(DATES, B, 256, LANES),
        cloud_free.reshape(T, STRIPS, LANES),
        jnp.asarray(gram),
        jnp.asarray(fit),
    )
    coef, share = pl.pallas_call(
        handed_on,
        out_shape=results,
        in_specs=[anywhere] * 2,
        out_specs=(anywhere, anywhere),
        scratch_shapes=[
            vmem((K, B, STRIPS, LANES), F32),
            vmem((B, T), F32),
            dma((2, K + 1)),
        ],
    )(coef, share)
    return coef.reshape(K, B, STRIPS, 1, LANES), share.T


def solution(mesh):
    return jax.shard_map(
        on_device,
        mesh=mesh,
        in_specs=(P("ta", None, "sa", None, None), P(None, None, ("ta", "sa"), None)),
        out_specs=(P(None, None, None, ("ta", "sa"), None), P()),
        check_vma=False,
    )
```

```python
import math

import jax
import jax.numpy as jnp
import numpy as np
from jax import lax
from jax.experimental import pallas as pl
from jax.experimental.pallas import tpu as pltpu
from jax.sharding import PartitionSpec as P

T = 120
HALF = 60
B = 4
K = 8
STRIPS = 32
LANES = 128
N_TA = 8
N_SA = 32
N_Y = 4
N_Z = 8
DATES = T // N_TA
TB = 24
MOMENTS = 21
GROUP = 3
GROUP_ROWS = (3, 1, 1, 2, 2)
COUNTS = 0
VMEM_LIMIT = 62 * 2**20
RIDGE = 1.0
CAUCHY = 4.0
TINY = 1e-6
MESH = pl.DeviceIdType.MESH
F32 = jnp.float32
BF16 = jnp.bfloat16


def basis_table():
    p = (np.arange(T, dtype=np.float64) + 0.5) / T
    q = 2.0 * p - 1.0
    columns = [np.ones_like(p), q]
    for h in range(1, 7):
        columns += [np.cos(2.0 * math.pi * h * p), np.sin(2.0 * math.pi * h * p)]
    columns.append(q * q)
    for h in range(1, 4):
        columns += [q * np.cos(2.0 * math.pi * h * p), q * np.sin(2.0 * math.pi * h * p)]
    return np.stack(columns, axis=1)


def two_parts(table):
    high = table.astype(np.float32).astype(BF16)
    low = (table - high.astype(np.float64)).astype(np.float32).astype(BF16)
    return high, low


def tables():
    x = basis_table()
    eye = np.eye(8)
    high, low = two_parts(np.kron(x.T, eye))
    gram = np.concatenate([high, low], axis=0)
    dh, dl = two_parts(np.kron(x[:, :K], eye))
    fit = np.concatenate([dh, dh, dl], axis=1)
    return gram, fit


def gram_entry(m, i, j):
    if j == 0:
        return m[i]
    if j == 1:
        return m[14] if i == 1 else m[13 + i]
    a, b = i // 2, j // 2

    def sine(k):
        if k == 0:
            return None
        return m[2 * k + 1] if k > 0 else -m[-2 * k + 1]

    if i % 2 == 0 and j % 2 == 0:
        return 0.5 * (m[2 * (a - b)] + m[2 * (a + b)])
    if i % 2 == 1 and j % 2 == 1:
        return 0.5 * (m[2 * (a - b)] - m[2 * (a + b)])
    cos_h, sin_h = (a, b) if i % 2 == 0 else (b, a)
    other = sine(sin_h - cos_h)
    return 0.5 * m[2 * (a + b) + 1] if other is None else 0.5 * (m[2 * (a + b) + 1] + other)


def factor(m):
    lower, plain, inverse = {}, {}, []
    for j in range(K):
        for i in range(j, K):
            e = gram_entry(m, i, j)
            if i == j:
                e = e + RIDGE
            for k in range(j):
                e = e - lower[i, k] * plain[j, k]
            plain[i, j] = e
        inverse.append(1.0 / plain[j, j])
        for i in range(j + 1, K):
            lower[i, j] = plain[i, j] * inverse[j]
    return lower, inverse


def solve(lower, inverse, rhs):
    y = []
    for i in range(K):
        e = rhs[i]
        for k in range(i):
            e = e - lower[i, k] * y[k]
        y.append(e)
    x = [None] * K
    for i in reversed(range(K)):
        e = y[i] * inverse[i]
        for k in range(i + 1, K):
            e = e - lower[k, i] * x[k]
        x[i] = e
    return x


def dot(a, b):
    return jnp.dot(a, b, preferred_element_type=F32)


def rows(x):
    n = x.shape[0]
    return jnp.concatenate(
        [x[:, :8].reshape(n * 8, LANES), x[:, 8:].reshape(n * 8, LANES)], axis=1
    )


def blocks(x):
    n = x.shape[0] // 8
    return x[:, :LANES].reshape(n, 8, LANES), x[:, LANES:].reshape(n, 8, LANES)


def halves(x):
    high = x.astype(BF16)
    return high, (x - high.astype(F32)).astype(BF16)


def stacked(c):
    high, low = halves(c)
    return jnp.concatenate([high, low, high], axis=0)


def lane_sums(x):
    ones = jnp.ones((8, LANES), F32)
    out = lax.dot_general(
        ones, x, (((1,), (1,)), ((), ())), precision=lax.Precision.HIGHEST,
        preferred_element_type=F32,
    )
    return out[0:1]


def kernel(
    scn, msk, gram_in, fit_in, coef, share,
    val, mraw, pk, mrecv, wf, rr, zh, zl, yh, yl, gram, fit, fac, mom, c1, dl, csend,
    sred, s8, near, far,
    bulk_s, bulk_r, local, msk_s, msk_r, near_s, near_r, far_s, far_r, cs, cr, own_c, here,
):
    ta = lax.axis_index("ta")
    sa = lax.axis_index("sa")

    def to_ta(k):
        return {"ta": lax.rem(ta + k, N_TA)}

    def to_sa(k):
        return {"sa": lax.rem(sa + k, N_SA)}

    mask_in = pltpu.make_async_copy(msk, mraw, local.at[0])
    mask_in.start()
    gram_copy = pltpu.make_async_copy(gram_in, gram, local.at[1])
    gram_copy.start()
    fit_copy = pltpu.make_async_copy(fit_in, fit, local.at[2])
    fit_copy.start()
    mine = pltpu.make_async_copy(
        scn.at[:, :, pl.ds(pl.multiple_of(ta * 32, 32), 32)],
        val.at[pl.ds(ta * DATES, DATES)],
        local.at[3],
    )
    mine.start()

    y, z = sa // N_Z, lax.rem(sa, N_Z)

    def beside(dy, dz):
        return {"sa": lax.rem(y + dy + N_Y, N_Y) * N_Z + lax.rem(z + dz + N_Z, N_Z)}

    barrier = pltpu.get_barrier_semaphore()
    for k in range(1, N_TA):
        pl.semaphore_signal(barrier, inc=1, device_id=to_ta(k), device_id_type=MESH)
    for dy, dz in ((0, 1), (0, -1), (1, 0), (-1, 0)):
        pl.semaphore_signal(barrier, inc=1, device_id=beside(dy, dz), device_id_type=MESH)
    pl.semaphore_wait(barrier, N_TA - 1 + 4)

    def send_bulk(b, start, size, at):
        for k in range(1, N_TA):
            t = lax.rem(ta + k, N_TA)
            pltpu.make_async_remote_copy(
                src_ref=scn.at[:, b, pl.ds(pl.multiple_of(t * 32 + start, 16), size)],
                dst_ref=val.at[pl.ds(ta * DATES, DATES), b, pl.ds(start, size)],
                send_sem=bulk_s.at[at],
                recv_sem=bulk_r.at[at],
                device_id={"ta": t},
                device_id_type=MESH,
            ).start()

    def send_band(b, carry):
        send_bulk(b, 0, 32, b)
        return carry

    lax.fori_loop(0, B - 1, send_band, 0)
    send_bulk(B - 1, 0, 16, B - 1)

    mask_in.wait()

    def pack(i, carry):
        t = i * 4
        pk[pl.ds(t, 4)] = mraw[pl.ds(t, 4)] + mraw[pl.ds(t + HALF, 4)] * 65536
        return carry

    lax.fori_loop(0, HALF // 4, pack, 0)

    for at, pair in enumerate((((0, 1), (0, -1)), ((0, 2), (0, -2)), ((1, 0), (-1, 0)), ((1, 0), (-1, 0)))):
        for dy, dz in pair:
            pl.semaphore_signal(here.at[at], inc=1, device_id=beside(dy, dz), device_id_type=MESH)
        pl.semaphore_wait(here.at[at], 2)

    def send_mask(k, carry):
        j = lax.rem(sa + k, N_SA)
        pltpu.make_async_remote_copy(
            src_ref=pk.at[:, pl.ds(j, 1)],
            dst_ref=mrecv.at[:, pl.ds(sa, 1)],
            send_sem=msk_s,
            recv_sem=msk_r,
            device_id={"sa": j},
            device_id_type=MESH,
        ).start()
        return carry

    lax.fori_loop(1, N_SA, send_mask, 0)
    mrecv[:, pl.ds(sa, 1)] = pk[:, pl.ds(sa, 1)]
    gram_copy.wait()
    fit_copy.wait()
    mine.wait()
    some_rows = mrecv.at[:, pl.ds(0, N_SA - 1)]
    pltpu.make_async_copy(some_rows, some_rows, msk_r).wait()

    def unpack(i, carry):
        t = i * 4
        both = mrecv[pl.ds(t, 4)]
        wf[pl.ds(t, 4)] = (both & 65535).astype(F32)
        wf[pl.ds(t + HALF, 4)] = (both >> 16).astype(F32)
        return carry

    lax.fori_loop(0, HALF // 4, unpack, 0)

    def near_send(g):
        group = pl.ds(GROUP * g, GROUP_ROWS[g])
        for k in range(1, N_TA):
            pltpu.make_async_remote_copy(
                src_ref=near.at[group, pl.ds(N_TA - 1, 1)], dst_ref=near.at[group, pl.ds(k - 1, 1)],
                send_sem=near_s.at[g], recv_sem=near_r.at[g],
                device_id=to_ta(k), device_id_type=MESH,
            ).start()

    def far_send(g):
        group = pl.ds(GROUP * g, GROUP_ROWS[g])
        others = near.at[group, pl.ds(0, N_TA - 1)]
        pltpu.make_async_copy(others, others, near_r.at[g]).wait()
        for r in range(GROUP_ROWS[g]):
            far[GROUP * g + r, pl.ds(N_SA - 1, 1)] = jnp.sum(near[GROUP * g + r], axis=0, keepdims=True)

        def send(k):
            pltpu.make_async_remote_copy(
                src_ref=far.at[group, pl.ds(N_SA - 1, 1)], dst_ref=far.at[group, pl.ds(k - 1, 1)],
                send_sem=far_s.at[g], recv_sem=far_r.at[g],
                device_id=to_sa(k), device_id_type=MESH,
            ).start()

        def send_three(k, carry):
            send(k)
            send(k + 10)
            send(k + 20)
            return carry

        lax.fori_loop(1, 11, send_three, 0)
        send(N_SA - 1)

    def far_wait(g):
        others = far.at[pl.ds(GROUP * g, GROUP_ROWS[g]), pl.ds(0, N_SA - 1)]
        pltpu.make_async_copy(others, others, far_r.at[g]).wait()

    def far_sum(row):
        return jnp.sum(far[row], axis=0, keepdims=True)

    sred[pl.ds(T, 8)] = jnp.zeros((8, LANES), F32)
    for q in range(T // TB):
        w = wf[pl.ds(q * TB, TB)]
        w = (w[:, :8] + w[:, 8:16]) + (w[:, 16:24] + w[:, 24:])
        sred[pl.ds(q * TB, TB)] = jnp.sum(w, axis=1)
    near[COUNTS, pl.ds(N_TA - 1, 1)] = lane_sums(sred[...])

    for h in range(2):
        for q in range(T // TB):
            zh[pl.ds(q * TB * 8, TB * 8)] = rows(
                wf[pl.ds(q * TB, TB), pl.ds(16 * h, 16)]
            ).astype(BF16)
        m = dot(gram[...], zh[...])
        m = m[: 8 * MOMENTS] + m[8 * MOMENTS :]
        lower, inverse = factor([m[8 * i : 8 * i + 8] for i in range(MOMENTS)])
        at = 0
        for j in range(K):
            for i in range(j + 1, K):
                fac[h, at] = lower[i, j]
                at += 1
        for j in range(K):
            fac[h, at + j] = inverse[j]

    def stored_factor(h):
        lower, at = {}, 0
        for j in range(K):
            for i in range(j + 1, K):
                lower[i, j] = fac[h, at]
                at += 1
        return lower, [fac[h, at + j] for j in range(K)]

    some_dates = T - DATES

    def wait_bulk(b, h, sem):
        if h == 0:
            @pl.when(b < B - 1)
            def _():
                part = val.at[pl.ds(0, some_dates), b]
                pltpu.make_async_copy(part, part, sem.at[b]).wait()

        @pl.when(b == B - 1)
        def _():
            part = val.at[pl.ds(0, some_dates), b, pl.ds(16 * h, 16)]
            pltpu.make_async_copy(part, part, sem.at[B - 1 + h]).wait()

    def squares_row(b):
        return jnp.where(b < 2, b + 1, GROUP * (b - 1))

    def tally_row(b):
        return GROUP * 3 + b + b // 2

    def first_pass(b):
        for h in range(2):
            wait_bulk(b, h, bulk_r)
            for q in range(T // TB):
                v = val[pl.ds(q * TB, TB), b, pl.ds(16 * h, 16)].astype(F32)
                w = wf[pl.ds(q * TB, TB), pl.ds(16 * h, 16)]
                zh[pl.ds(q * TB * 8, TB * 8)] = rows(v * w).astype(BF16)
            table = jnp.concatenate(
                [gram[0 : 8 * K], gram[8 * MOMENTS : 8 * MOMENTS + 8 * K]], axis=0
            )
            m = dot(table, zh[...])
            m = m[: 8 * K] + m[8 * K :]
            lower, inverse = stored_factor(h)
            c = solve(lower, inverse, [m[8 * i : 8 * i + 8] for i in range(K)])
            c = jnp.concatenate(c, axis=0)
            c1[b, h] = c
            cc = stacked(c)
            for q in range(T // TB):
                v = val[pl.ds(q * TB, TB), b, pl.ds(16 * h, 16)].astype(F32)
                f0, f1 = blocks(dot(fit[pl.ds(q * TB * 8, TB * 8)], cc))
                r0, r1 = v[:, :8] - f0, v[:, 8:] - f1
                w = wf[pl.ds(q * TB, TB), pl.ds(16 * h, 16)]
                rr[b, pl.ds(q * TB, TB), pl.ds(16 * h, 8)] = r0
                rr[b, pl.ds(q * TB, TB), pl.ds(16 * h + 8, 8)] = r1
                total = jnp.sum(w[:, :8] * (r0 * r0) + w[:, 8:] * (r1 * r1), axis=1)
                if h == 0:
                    sred[pl.ds(q * TB, TB)] = total
                else:
                    sred[pl.ds(q * TB, TB)] += total
        near[squares_row(b), pl.ds(N_TA - 1, 1)] = lane_sums(sred[...])

    def send_coefs(b):
        def send(k, carry):
            j = lax.rem(sa + k, N_SA)
            pltpu.make_async_remote_copy(
                src_ref=csend.at[:, b, pl.ds(j, 1)],
                dst_ref=coef.at[:, b, pl.ds(sa, 1)],
                send_sem=cs.at[b],
                recv_sem=cr.at[b],
                device_id={"sa": j},
                device_id_type=MESH,
            ).start()
            return carry

        lax.fori_loop(1, N_SA, send, 0)
        pltpu.make_async_copy(
            csend.at[:, b, pl.ds(sa, 1)], coef.at[:, b, pl.ds(sa, 1)], own_c.at[b]
        ).start()

    def second_pass(b):
        spread = CAUCHY * (far_sum(squares_row(b)) + TINY) / (far_sum(COUNTS) + 1.0)
        column = jnp.transpose(jnp.broadcast_to(spread, (LANES, LANES)))
        s8[...] = jnp.broadcast_to(column[:T].reshape(T, 1, LANES), (T, 8, LANES))

        for h in range(2):
            for q in range(T // TB):
                dates = pl.ds(q * TB, TB)
                s = s8[dates]
                parts = []
                for g in range(2):
                    at = pl.ds(16 * h + 8 * g, 8)
                    r = rr[b, dates, at]
                    robust = wf[dates, at] * s / (s + r * r)
                    parts.append((robust.reshape(TB * 8, LANES), (robust * r).reshape(TB * 8, LANES)))
                z = jnp.concatenate([parts[0][0], parts[1][0]], axis=1)
                y = jnp.concatenate([parts[0][1], parts[1][1]], axis=1)
                out = pl.ds(q * TB * 8, TB * 8)
                zh[out], zl[out] = halves(z)
                yh[out], yl[out] = halves(y)
            m = dot(gram[...], zh[...])
            m = m[: 8 * MOMENTS] + m[8 * MOMENTS :] + dot(gram[: 8 * MOMENTS], zl[...])
            mom[h, pl.ds(0, 8 * MOMENTS)] = m
            table = jnp.concatenate(
                [gram[0 : 8 * K], gram[8 * MOMENTS : 8 * MOMENTS + 8 * K]], axis=0
            )
            m = dot(table, yh[...])
            m = m[: 8 * K] + m[8 * K :] + dot(gram[: 8 * K], yl[...])
            mom[h, pl.ds(8 * MOMENTS, 8 * K)] = m - c1[b, h]

        def both(at):
            return jnp.concatenate([mom[0, pl.ds(at, 8)], mom[1, pl.ds(at, 8)]], axis=1)

        lower, inverse = factor([both(8 * k) for k in range(MOMENTS)])
        d = solve(lower, inverse, [both(8 * (MOMENTS + k)) for k in range(K)])
        for k in range(K):
            for h in range(2):
                part = d[k][:, 256 * h : 256 * h + 256]
                dl[h, pl.ds(8 * k, 8)] = part
                c = c1[b, h, pl.ds(8 * k, 8)] + part
                csend[k, b, pl.ds(16 * h, 8)] = c[:, :LANES]
                csend[k, b, pl.ds(16 * h + 8, 8)] = c[:, LANES:]

        @pl.when(b == B - 1)
        def _():
            send_coefs(b)

        for h in range(2):
            cc = stacked(dl[h])
            for q in range(T // TB):
                dates = pl.ds(q * TB, TB)
                f = blocks(dot(fit[pl.ds(q * TB * 8, TB * 8)], cc))
                s = s8[dates]
                terms = []
                for g in range(2):
                    at = pl.ds(16 * h + 8 * g, 8)
                    e = rr[b, dates, at] - f[g]
                    e = e * e
                    terms.append(wf[dates, at] * e / (e + s))
                part = jnp.sum(terms[0] + terms[1], axis=1)
                if h == 0:
                    sred[dates] = part
                else:
                    sred[dates] += part
        near[tally_row(b), pl.ds(N_TA - 1, 1)] = lane_sums(sred[...])

    def step(i, carry):
        @pl.when((i < 3) | (i == 4))
        def _():
            first_pass(jnp.where(i < 3, i, B - 1))

        @pl.when(i == 1)
        def _():
            near_send(0)
            send_bulk(B - 1, 16, 16, B)

        @pl.when(i == 2)
        def _():
            near_send(1)

        @pl.when(i == 3)
        def _():
            far_send(0)

        @pl.when(i == 4)
        def _():
            near_send(2)
            far_send(1)

        @pl.when(i == 5)
        def _():
            far_wait(0)

        @pl.when(i == 7)
        def _():
            far_wait(1)

        @pl.when(i == 8)
        def _():
            far_wait(2)

        @pl.when(i >= 5)
        def _():
            second_pass(i - 5)

        @pl.when(i == 5)
        def _():
            far_send(2)

        @pl.when((i >= 5) & (i < 8))
        def _():
            send_coefs(i - 5)

        @pl.when(i == 6)
        def _():
            near_send(3)

        @pl.when(i == 7)
        def _():
            far_send(3)

        return carry

    lax.fori_loop(0, 9, step, 0)
    near_send(4)
    far_send(4)
    far_wait(3)
    far_wait(4)
    for b in range(B):
        share[b : b + 1] = (far_sum(tally_row(b)) / (far_sum(COUNTS) + 1.0))[:, :T]

    def finish(b, carry):
        wait_bulk(b, 0, bulk_s)
        wait_bulk(b, 1, bulk_s)
        some_coefs = coef.at[:, b, pl.ds(0, N_SA - 1)]
        pltpu.make_async_copy(some_coefs, some_coefs, cr.at[b]).wait()
        pltpu.make_async_copy(some_coefs, some_coefs, cs.at[b]).wait()
        pltpu.make_async_copy(
            csend.at[:, b, pl.ds(sa, 1)], coef.at[:, b, pl.ds(sa, 1)], own_c.at[b]
        ).wait()
        return carry

    lax.fori_loop(0, B, finish, 0)
    pltpu.make_async_copy(some_rows, some_rows, msk_s).wait()

    for g, n in enumerate(GROUP_ROWS):
        rows_near = near.at[pl.ds(GROUP * g, n), pl.ds(0, N_TA - 1)]
        pltpu.make_async_copy(rows_near, rows_near, near_s.at[g]).wait()
        rows_far = far.at[pl.ds(GROUP * g, n), pl.ds(0, N_SA - 1)]
        pltpu.make_async_copy(rows_far, rows_far, far_s.at[g]).wait()


def handed_on(coef_in, share_in, coef_out, share_out, coef, share, sems):
    arrays = [(coef_in.at[k], coef.at[k], coef_out.at[k]) for k in range(K)]
    arrays.append((share_in, share, share_out))
    for i, (source, held, _) in enumerate(arrays):
        pltpu.make_async_copy(source, held, sems.at[0, i]).start()
    for i, (source, held, target) in enumerate(arrays):
        pltpu.make_async_copy(source, held, sems.at[0, i]).wait()
        pltpu.make_async_copy(held, target, sems.at[1, i]).start()
    for i, (_, held, target) in enumerate(arrays):
        pltpu.make_async_copy(held, target, sems.at[1, i]).wait()


def on_device(scenes, cloud_free):
    gram, fit = tables()
    vmem = pltpu.VMEM
    dma = pltpu.SemaphoreType.DMA
    results = (
        jax.ShapeDtypeStruct((K, B, STRIPS, LANES), F32),
        jax.ShapeDtypeStruct((B, T), F32),
    )
    anywhere = pl.BlockSpec(memory_space=pl.ANY)
    coef, share = pl.pallas_call(
        kernel,
        out_shape=results,
        in_specs=[anywhere] * 4,
        out_specs=(anywhere, pl.BlockSpec(memory_space=vmem)),
        scratch_shapes=[
            vmem((T, B, 32, LANES), BF16),
            vmem((T, 32, LANES), jnp.int32),
            vmem((HALF, 32, LANES), jnp.int32),
            vmem((HALF, 32, LANES), jnp.int32),
            vmem((T, 32, LANES), F32),
            vmem((B, T, 32, LANES), F32),
            vmem((T * 8, 256), BF16),
            vmem((T * 8, 256), BF16),
            vmem((T * 8, 256), BF16),
            vmem((T * 8, 256), BF16),
            vmem(gram.shape, BF16),
            vmem(fit.shape, BF16),
            vmem((2, 36, 8, 256), F32),
            vmem((2, 8 * (MOMENTS + K), 256), F32),
            vmem((B, 2, 8 * K, 256), F32),
            vmem((2, 8 * K, 256), F32),
            vmem((K, B, 32, LANES), F32),
            vmem((LANES, LANES), F32),
            vmem((T, 8, LANES), F32),
            vmem((GROUP * len(GROUP_ROWS), N_TA, LANES), F32),
            vmem((GROUP * len(GROUP_ROWS), N_SA, LANES), F32),
            dma((B + 1,)),
            dma((B + 1,)),
            dma((4,)),
            dma,
            dma,
            dma((len(GROUP_ROWS),)),
            dma((len(GROUP_ROWS),)),
            dma((len(GROUP_ROWS),)),
            dma((len(GROUP_ROWS),)),
            dma((B,)),
            dma((B,)),
            dma((B,)),
            pltpu.SemaphoreType.REGULAR((4,)),
        ],
        compiler_params=pltpu.CompilerParams(
            collective_id=0, has_side_effects=True, vmem_limit_bytes=VMEM_LIMIT
        ),
    )(
        scenes.reshape(DATES, B, 256, LANES),
        cloud_free.reshape(T, STRIPS, LANES),
        jnp.asarray(gram),
        jnp.asarray(fit),
    )
    coef, share = pl.pallas_call(
        handed_on,
        out_shape=results,
        in_specs=[anywhere] * 2,
        out_specs=(anywhere, anywhere),
        scratch_shapes=[
            vmem((K, B, STRIPS, LANES), F32),
            vmem((B, T), F32),
            dma((2, K + 1)),
        ],
    )(coef, share)
    return coef.reshape(K, B, STRIPS, 1, LANES), share.T


def solution(mesh):
    return jax.shard_map(
        on_device,
        mesh=mesh,
        in_specs=(P("ta", None, "sa", None, None), P(None, None, ("ta", "sa"), None)),
        out_specs=(P(None, None, None, ("ta", "sa"), None), P()),
        check_vma=False,
    )
```

```python
import math

import jax
import jax.numpy as jnp
import numpy as np
from jax import lax
from jax.experimental import pallas as pl
from jax.experimental.pallas import tpu as pltpu
from jax.sharding import PartitionSpec as P

T = 120
HALF = 60
B = 4
K = 8
STRIPS = 32
LANES = 128
N_TA = 8
N_SA = 32
N_Y = 4
N_Z = 8
DATES = T // N_TA
TB = 24
MOMENTS = 21
GROUP = 3
GROUP_ROWS = (3, 1, 1, 2, 2)
COUNTS = 0
FAR_FIRST = (4, 5, 3, 2, 6, 7, 1)
VMEM_LIMIT = 62 * 2**20
RIDGE = 1.0
CAUCHY = 4.0
TINY = 1e-6
MESH = pl.DeviceIdType.MESH
F32 = jnp.float32
BF16 = jnp.bfloat16


def basis_table():
    p = (np.arange(T, dtype=np.float64) + 0.5) / T
    q = 2.0 * p - 1.0
    columns = [np.ones_like(p), q]
    for h in range(1, 7):
        columns += [np.cos(2.0 * math.pi * h * p), np.sin(2.0 * math.pi * h * p)]
    columns.append(q * q)
    for h in range(1, 4):
        columns += [q * np.cos(2.0 * math.pi * h * p), q * np.sin(2.0 * math.pi * h * p)]
    return np.stack(columns, axis=1)


def two_parts(table):
    high = table.astype(np.float32).astype(BF16)
    low = (table - high.astype(np.float64)).astype(np.float32).astype(BF16)
    return high, low


def tables():
    x = basis_table()
    eye = np.eye(8)
    high, low = two_parts(np.kron(x.T, eye))
    gram = np.concatenate([high, low], axis=0)
    dh, dl = two_parts(np.kron(x[:, :K], eye))
    fit = np.concatenate([dh, dh, dl], axis=1)
    return gram, fit


def gram_entry(m, i, j):
    if j == 0:
        return m[i]
    if j == 1:
        return m[14] if i == 1 else m[13 + i]
    a, b = i // 2, j // 2

    def sine(k):
        if k == 0:
            return None
        return m[2 * k + 1] if k > 0 else -m[-2 * k + 1]

    if i % 2 == 0 and j % 2 == 0:
        return 0.5 * (m[2 * (a - b)] + m[2 * (a + b)])
    if i % 2 == 1 and j % 2 == 1:
        return 0.5 * (m[2 * (a - b)] - m[2 * (a + b)])
    cos_h, sin_h = (a, b) if i % 2 == 0 else (b, a)
    other = sine(sin_h - cos_h)
    return 0.5 * m[2 * (a + b) + 1] if other is None else 0.5 * (m[2 * (a + b) + 1] + other)


def factor(m):
    lower, plain, inverse = {}, {}, []
    for j in range(K):
        for i in range(j, K):
            e = gram_entry(m, i, j)
            if i == j:
                e = e + RIDGE
            for k in range(j):
                e = e - lower[i, k] * plain[j, k]
            plain[i, j] = e
        inverse.append(1.0 / plain[j, j])
        for i in range(j + 1, K):
            lower[i, j] = plain[i, j] * inverse[j]
    return lower, inverse


def solve(lower, inverse, rhs):
    y = []
    for i in range(K):
        e = rhs[i]
        for k in range(i):
            e = e - lower[i, k] * y[k]
        y.append(e)
    x = [None] * K
    for i in reversed(range(K)):
        e = y[i] * inverse[i]
        for k in range(i + 1, K):
            e = e - lower[k, i] * x[k]
        x[i] = e
    return x


def dot(a, b):
    return jnp.dot(a, b, preferred_element_type=F32)


def rows(x):
    n = x.shape[0]
    return jnp.concatenate(
        [x[:, :8].reshape(n * 8, LANES), x[:, 8:].reshape(n * 8, LANES)], axis=1
    )


def blocks(x):
    n = x.shape[0] // 8
    return x[:, :LANES].reshape(n, 8, LANES), x[:, LANES:].reshape(n, 8, LANES)


def halves(x):
    high = x.astype(BF16)
    return high, (x - high.astype(F32)).astype(BF16)


def stacked(c):
    high, low = halves(c)
    return jnp.concatenate([high, low, high], axis=0)


def lane_sums(x):
    ones = jnp.ones((8, LANES), F32)
    out = lax.dot_general(
        ones, x, (((1,), (1,)), ((), ())), precision=lax.Precision.HIGHEST,
        preferred_element_type=F32,
    )
    return out[0:1]


def kernel(
    scn, msk, gram_in, fit_in, coef, share,
    val, mraw, pk, mrecv, wf, rr, zh, zl, yh, yl, gram, fit, fac, mom, c1, dl, csend,
    sred, s8, near, far,
    bulk_s, bulk_r, local, msk_s, msk_r, near_s, near_r, far_s, far_r, cs, cr, own_c, here,
):
    ta = lax.axis_index("ta")
    sa = lax.axis_index("sa")

    def to_ta(k):
        return {"ta": lax.rem(ta + k, N_TA)}

    def to_sa(k):
        return {"sa": lax.rem(sa + k, N_SA)}

    mask_in = pltpu.make_async_copy(msk, mraw, local.at[0])
    mask_in.start()
    gram_copy = pltpu.make_async_copy(gram_in, gram, local.at[1])
    gram_copy.start()
    fit_copy = pltpu.make_async_copy(fit_in, fit, local.at[2])
    fit_copy.start()
    mine = pltpu.make_async_copy(
        scn.at[:, :, pl.ds(pl.multiple_of(ta * 32, 32), 32)],
        val.at[pl.ds(ta * DATES, DATES)],
        local.at[3],
    )
    mine.start()

    y, z = sa // N_Z, lax.rem(sa, N_Z)

    def beside(dy, dz):
        return {"sa": lax.rem(y + dy + N_Y, N_Y) * N_Z + lax.rem(z + dz + N_Z, N_Z)}

    barrier = pltpu.get_barrier_semaphore()
    for k in range(1, N_TA):
        pl.semaphore_signal(barrier, inc=1, device_id=to_ta(k), device_id_type=MESH)
    for dy, dz in ((0, 1), (0, -1), (1, 0), (-1, 0)):
        pl.semaphore_signal(barrier, inc=1, device_id=beside(dy, dz), device_id_type=MESH)
    pl.semaphore_wait(barrier, N_TA - 1 + 4)

    def send_bulk(b, start, size, at):
        for k in FAR_FIRST:
            t = lax.rem(ta + k, N_TA)
            pltpu.make_async_remote_copy(
                src_ref=scn.at[:, b, pl.ds(pl.multiple_of(t * 32 + start, 16), size)],
                dst_ref=val.at[pl.ds(ta * DATES, DATES), b, pl.ds(start, size)],
                send_sem=bulk_s.at[at],
                recv_sem=bulk_r.at[at],
                device_id={"ta": t},
                device_id_type=MESH,
            ).start()

    def send_band(b, carry):
        send_bulk(b, 0, 32, b)
        return carry

    lax.fori_loop(0, B - 1, send_band, 0)
    send_bulk(B - 1, 0, 16, B - 1)

    mask_in.wait()

    def pack(i, carry):
        t = i * 4
        pk[pl.ds(t, 4)] = mraw[pl.ds(t, 4)] + mraw[pl.ds(t + HALF, 4)] * 65536
        return carry

    lax.fori_loop(0, HALF // 4, pack, 0)

    for at, pair in enumerate((((0, 1), (0, -1)), ((0, 2), (0, -2)), ((1, 0), (-1, 0)), ((1, 0), (-1, 0)))):
        for dy, dz in pair:
            pl.semaphore_signal(here.at[at], inc=1, device_id=beside(dy, dz), device_id_type=MESH)
        pl.semaphore_wait(here.at[at], 2)

    def send_mask(k, carry):
        j = lax.rem(sa + k, N_SA)
        pltpu.make_async_remote_copy(
            src_ref=pk.at[:, pl.ds(j, 1)],
            dst_ref=mrecv.at[:, pl.ds(sa, 1)],
            send_sem=msk_s,
            recv_sem=msk_r,
            device_id={"sa": j},
            device_id_type=MESH,
        ).start()
        return carry

    lax.fori_loop(1, N_SA, send_mask, 0)
    mrecv[:, pl.ds(sa, 1)] = pk[:, pl.ds(sa, 1)]
    gram_copy.wait()
    fit_copy.wait()
    mine.wait()
    some_rows = mrecv.at[:, pl.ds(0, N_SA - 1)]
    pltpu.make_async_copy(some_rows, some_rows, msk_r).wait()

    def unpack(i, carry):
        t = i * 4
        both = mrecv[pl.ds(t, 4)]
        wf[pl.ds(t, 4)] = (both & 65535).astype(F32)
        wf[pl.ds(t + HALF, 4)] = (both >> 16).astype(F32)
        return carry

    lax.fori_loop(0, HALF // 4, unpack, 0)

    def near_send(g):
        group = pl.ds(GROUP * g, GROUP_ROWS[g])
        for k in range(1, N_TA):
            pltpu.make_async_remote_copy(
                src_ref=near.at[group, pl.ds(N_TA - 1, 1)], dst_ref=near.at[group, pl.ds(k - 1, 1)],
                send_sem=near_s.at[g], recv_sem=near_r.at[g],
                device_id=to_ta(k), device_id_type=MESH,
            ).start()

    def far_send(g):
        group = pl.ds(GROUP * g, GROUP_ROWS[g])
        others = near.at[group, pl.ds(0, N_TA - 1)]
        pltpu.make_async_copy(others, others, near_r.at[g]).wait()
        for r in range(GROUP_ROWS[g]):
            far[GROUP * g + r, pl.ds(N_SA - 1, 1)] = jnp.sum(near[GROUP * g + r], axis=0, keepdims=True)

        def send(k):
            pltpu.make_async_remote_copy(
                src_ref=far.at[group, pl.ds(N_SA - 1, 1)], dst_ref=far.at[group, pl.ds(k - 1, 1)],
                send_sem=far_s.at[g], recv_sem=far_r.at[g],
                device_id=to_sa(k), device_id_type=MESH,
            ).start()

        def send_six(k, carry):
            for more in range(0, 30, 5):
                send(k + more)
            return carry

        lax.fori_loop(1, 6, send_six, 0)
        send(N_SA - 1)

    def far_wait(g):
        others = far.at[pl.ds(GROUP * g, GROUP_ROWS[g]), pl.ds(0, N_SA - 1)]
        pltpu.make_async_copy(others, others, far_r.at[g]).wait()

    def far_sum(row):
        return jnp.sum(far[row], axis=0, keepdims=True)

    sred[pl.ds(T, 8)] = jnp.zeros((8, LANES), F32)
    for q in range(T // TB):
        w = wf[pl.ds(q * TB, TB)]
        w = (w[:, :8] + w[:, 8:16]) + (w[:, 16:24] + w[:, 24:])
        sred[pl.ds(q * TB, TB)] = jnp.sum(w, axis=1)
    near[COUNTS, pl.ds(N_TA - 1, 1)] = lane_sums(sred[...])

    for h in range(2):
        for q in range(T // TB):
            zh[pl.ds(q * TB * 8, TB * 8)] = rows(
                wf[pl.ds(q * TB, TB), pl.ds(16 * h, 16)]
            ).astype(BF16)
        m = dot(gram[...], zh[...])
        m = m[: 8 * MOMENTS] + m[8 * MOMENTS :]
        lower, inverse = factor([m[8 * i : 8 * i + 8] for i in range(MOMENTS)])
        at = 0
        for j in range(K):
            for i in range(j + 1, K):
                fac[h, at] = lower[i, j]
                at += 1
        for j in range(K):
            fac[h, at + j] = inverse[j]

    def stored_factor(h):
        lower, at = {}, 0
        for j in range(K):
            for i in range(j + 1, K):
                lower[i, j] = fac[h, at]
                at += 1
        return lower, [fac[h, at + j] for j in range(K)]

    some_dates = T - DATES

    def wait_bulk(b, h, sem):
        if h == 0:
            @pl.when(b < B - 1)
            def _():
                part = val.at[pl.ds(0, some_dates), b]
                pltpu.make_async_copy(part, part, sem.at[b]).wait()

        @pl.when(b == B - 1)
        def _():
            part = val.at[pl.ds(0, some_dates), b, pl.ds(16 * h, 16)]
            pltpu.make_async_copy(part, part, sem.at[B - 1 + h]).wait()

    def squares_row(b):
        return jnp.where(b < 2, b + 1, GROUP * (b - 1))

    def tally_row(b):
        return GROUP * 3 + b + b // 2

    def first_pass(b):
        for h in range(2):
            wait_bulk(b, h, bulk_r)
            for q in range(T // TB):
                v = val[pl.ds(q * TB, TB), b, pl.ds(16 * h, 16)].astype(F32)
                w = wf[pl.ds(q * TB, TB), pl.ds(16 * h, 16)]
                zh[pl.ds(q * TB * 8, TB * 8)] = rows(v * w).astype(BF16)
            table = jnp.concatenate(
                [gram[0 : 8 * K], gram[8 * MOMENTS : 8 * MOMENTS + 8 * K]], axis=0
            )
            m = dot(table, zh[...])
            m = m[: 8 * K] + m[8 * K :]
            lower, inverse = stored_factor(h)
            c = solve(lower, inverse, [m[8 * i : 8 * i + 8] for i in range(K)])
            c = jnp.concatenate(c, axis=0)
            c1[b, h] = c
            cc = stacked(c)
            for q in range(T // TB):
                v = val[pl.ds(q * TB, TB), b, pl.ds(16 * h, 16)].astype(F32)
                f0, f1 = blocks(dot(fit[pl.ds(q * TB * 8, TB * 8)], cc))
                r0, r1 = v[:, :8] - f0, v[:, 8:] - f1
                w = wf[pl.ds(q * TB, TB), pl.ds(16 * h, 16)]
                rr[b, pl.ds(q * TB, TB), pl.ds(16 * h, 8)] = r0
                rr[b, pl.ds(q * TB, TB), pl.ds(16 * h + 8, 8)] = r1
                total = jnp.sum(w[:, :8] * (r0 * r0) + w[:, 8:] * (r1 * r1), axis=1)
                if h == 0:
                    sred[pl.ds(q * TB, TB)] = total
                else:
                    sred[pl.ds(q * TB, TB)] += total
        near[squares_row(b), pl.ds(N_TA - 1, 1)] = lane_sums(sred[...])

    def send_coefs(b):
        def send(k):
            j = lax.rem(sa + k, N_SA)
            pltpu.make_async_remote_copy(
                src_ref=csend.at[:, b, pl.ds(j, 1)],
                dst_ref=coef.at[:, b, pl.ds(sa, 1)],
                send_sem=cs.at[b],
                recv_sem=cr.at[b],
                device_id={"sa": j},
                device_id_type=MESH,
            ).start()

        def send_six(k, carry):
            for more in range(0, 30, 5):
                send(k + more)
            return carry

        lax.fori_loop(1, 6, send_six, 0)
        send(N_SA - 1)
        pltpu.make_async_copy(
            csend.at[:, b, pl.ds(sa, 1)], coef.at[:, b, pl.ds(sa, 1)], own_c.at[b]
        ).start()

    def second_pass(b):
        spread = CAUCHY * (far_sum(squares_row(b)) + TINY) / (far_sum(COUNTS) + 1.0)
        column = jnp.transpose(jnp.broadcast_to(spread, (LANES, LANES)))
        s8[...] = jnp.broadcast_to(column[:T].reshape(T, 1, LANES), (T, 8, LANES))

        for h in range(2):
            for q in range(T // TB):
                dates = pl.ds(q * TB, TB)
                s = s8[dates]
                parts = []
                for g in range(2):
                    at = pl.ds(16 * h + 8 * g, 8)
                    r = rr[b, dates, at]
                    robust = wf[dates, at] * s / (s + r * r)
                    parts.append((robust.reshape(TB * 8, LANES), (robust * r).reshape(TB * 8, LANES)))
                z = jnp.concatenate([parts[0][0], parts[1][0]], axis=1)
                y = jnp.concatenate([parts[0][1], parts[1][1]], axis=1)
                out = pl.ds(q * TB * 8, TB * 8)
                zh[out], zl[out] = halves(z)
                yh[out], yl[out] = halves(y)
            m = dot(gram[...], zh[...])
            m = m[: 8 * MOMENTS] + m[8 * MOMENTS :] + dot(gram[: 8 * MOMENTS], zl[...])
            mom[h, pl.ds(0, 8 * MOMENTS)] = m
            table = jnp.concatenate(
                [gram[0 : 8 * K], gram[8 * MOMENTS : 8 * MOMENTS + 8 * K]], axis=0
            )
            m = dot(table, yh[...])
            m = m[: 8 * K] + m[8 * K :] + dot(gram[: 8 * K], yl[...])
            mom[h, pl.ds(8 * MOMENTS, 8 * K)] = m - c1[b, h]

        def both(at):
            return jnp.concatenate([mom[0, pl.ds(at, 8)], mom[1, pl.ds(at, 8)]], axis=1)

        lower, inverse = factor([both(8 * k) for k in range(MOMENTS)])
        d = solve(lower, inverse, [both(8 * (MOMENTS + k)) for k in range(K)])
        for k in range(K):
            for h in range(2):
                part = d[k][:, 256 * h : 256 * h + 256]
                dl[h, pl.ds(8 * k, 8)] = part
                c = c1[b, h, pl.ds(8 * k, 8)] + part
                csend[k, b, pl.ds(16 * h, 8)] = c[:, :LANES]
                csend[k, b, pl.ds(16 * h + 8, 8)] = c[:, LANES:]

        @pl.when(b == B - 1)
        def _():
            send_coefs(b)

        for h in range(2):
            cc = stacked(dl[h])
            for q in range(T // TB):
                dates = pl.ds(q * TB, TB)
                f = blocks(dot(fit[pl.ds(q * TB * 8, TB * 8)], cc))
                s = s8[dates]
                terms = []
                for g in range(2):
                    at = pl.ds(16 * h + 8 * g, 8)
                    e = rr[b, dates, at] - f[g]
                    e = e * e
                    terms.append(wf[dates, at] * e / (e + s))
                part = jnp.sum(terms[0] + terms[1], axis=1)
                if h == 0:
                    sred[dates] = part
                else:
                    sred[dates] += part
        near[tally_row(b), pl.ds(N_TA - 1, 1)] = lane_sums(sred[...])

    def step(i, carry):
        @pl.when((i < 3) | (i == 4))
        def _():
            first_pass(jnp.where(i < 3, i, B - 1))

        @pl.when(i == 1)
        def _():
            near_send(0)
            send_bulk(B - 1, 16, 16, B)

        @pl.when(i == 2)
        def _():
            near_send(1)

        @pl.when(i == 3)
        def _():
            far_send(0)

        @pl.when(i == 4)
        def _():
            near_send(2)
            far_send(1)

        @pl.when(i == 5)
        def _():
            far_wait(0)

        @pl.when(i == 7)
        def _():
            far_wait(1)

        @pl.when(i == 8)
        def _():
            far_wait(2)

        @pl.when(i >= 5)
        def _():
            second_pass(i - 5)

        @pl.when(i == 5)
        def _():
            far_send(2)

        @pl.when((i >= 5) & (i < 8))
        def _():
            send_coefs(i - 5)

        @pl.when(i == 6)
        def _():
            near_send(3)

        return carry

    lax.fori_loop(0, 9, step, 0)
    near_send(4)
    far_send(3)
    far_send(4)
    far_wait(3)
    far_wait(4)
    for b in range(B):
        share[b : b + 1] = (far_sum(tally_row(b)) / (far_sum(COUNTS) + 1.0))[:, :T]

    def finish(b, carry):
        wait_bulk(b, 0, bulk_s)
        wait_bulk(b, 1, bulk_s)
        some_coefs = coef.at[:, b, pl.ds(0, N_SA - 1)]
        pltpu.make_async_copy(some_coefs, some_coefs, cr.at[b]).wait()
        pltpu.make_async_copy(some_coefs, some_coefs, cs.at[b]).wait()
        pltpu.make_async_copy(
            csend.at[:, b, pl.ds(sa, 1)], coef.at[:, b, pl.ds(sa, 1)], own_c.at[b]
        ).wait()
        return carry

    lax.fori_loop(0, B, finish, 0)
    pltpu.make_async_copy(some_rows, some_rows, msk_s).wait()

    for g, n in enumerate(GROUP_ROWS):
        rows_near = near.at[pl.ds(GROUP * g, n), pl.ds(0, N_TA - 1)]
        pltpu.make_async_copy(rows_near, rows_near, near_s.at[g]).wait()
        rows_far = far.at[pl.ds(GROUP * g, n), pl.ds(0, N_SA - 1)]
        pltpu.make_async_copy(rows_far, rows_far, far_s.at[g]).wait()


def handed_on(coef_in, share_in, coef_out, share_out, coef, share, sems):
    arrays = [(coef_in.at[k], coef.at[k], coef_out.at[k]) for k in range(K)]
    arrays.append((share_in, share, share_out))
    for i, (source, held, _) in enumerate(arrays):
        pltpu.make_async_copy(source, held, sems.at[0, i]).start()
    for i, (source, held, target) in enumerate(arrays):
        pltpu.make_async_copy(source, held, sems.at[0, i]).wait()
        pltpu.make_async_copy(held, target, sems.at[1, i]).start()
    for i, (_, held, target) in enumerate(arrays):
        pltpu.make_async_copy(held, target, sems.at[1, i]).wait()


def on_device(scenes, cloud_free):
    gram, fit = tables()
    vmem = pltpu.VMEM
    dma = pltpu.SemaphoreType.DMA
    results = (
        jax.ShapeDtypeStruct((K, B, STRIPS, LANES), F32),
        jax.ShapeDtypeStruct((B, T), F32),
    )
    anywhere = pl.BlockSpec(memory_space=pl.ANY)
    coef, share = pl.pallas_call(
        kernel,
        out_shape=results,
        in_specs=[anywhere] * 4,
        out_specs=(anywhere, pl.BlockSpec(memory_space=vmem)),
        scratch_shapes=[
            vmem((T, B, 32, LANES), BF16),
            vmem((T, 32, LANES), jnp.int32),
            vmem((HALF, 32, LANES), jnp.int32),
            vmem((HALF, 32, LANES), jnp.int32),
            vmem((T, 32, LANES), F32),
            vmem((B, T, 32, LANES), F32),
            vmem((T * 8, 256), BF16),
            vmem((T * 8, 256), BF16),
            vmem((T * 8, 256), BF16),
            vmem((T * 8, 256), BF16),
            vmem(gram.shape, BF16),
            vmem(fit.shape, BF16),
            vmem((2, 36, 8, 256), F32),
            vmem((2, 8 * (MOMENTS + K), 256), F32),
            vmem((B, 2, 8 * K, 256), F32),
            vmem((2, 8 * K, 256), F32),
            vmem((K, B, 32, LANES), F32),
            vmem((LANES, LANES), F32),
            vmem((T, 8, LANES), F32),
            vmem((GROUP * len(GROUP_ROWS), N_TA, LANES), F32),
            vmem((GROUP * len(GROUP_ROWS), N_SA, LANES), F32),
            dma((B + 1,)),
            dma((B + 1,)),
            dma((4,)),
            dma,
            dma,
            dma((len(GROUP_ROWS),)),
            dma((len(GROUP_ROWS),)),
            dma((len(GROUP_ROWS),)),
            dma((len(GROUP_ROWS),)),
            dma((B,)),
            dma((B,)),
            dma((B,)),
            pltpu.SemaphoreType.REGULAR((4,)),
        ],
        compiler_params=pltpu.CompilerParams(
            collective_id=0, has_side_effects=True, vmem_limit_bytes=VMEM_LIMIT
        ),
    )(
        scenes.reshape(DATES, B, 256, LANES),
        cloud_free.reshape(T, STRIPS, LANES),
        jnp.asarray(gram),
        jnp.asarray(fit),
    )
    coef, share = pl.pallas_call(
        handed_on,
        out_shape=results,
        in_specs=[anywhere] * 2,
        out_specs=(anywhere, anywhere),
        scratch_shapes=[
            vmem((K, B, STRIPS, LANES), F32),
            vmem((B, T), F32),
            dma((2, K + 1)),
        ],
    )(coef, share)
    return coef.reshape(K, B, STRIPS, 1, LANES), share.T


def solution(mesh):
    return jax.shard_map(
        on_device,
        mesh=mesh,
        in_specs=(P("ta", None, "sa", None, None), P(None, None, ("ta", "sa"), None)),
        out_specs=(P(None, None, None, ("ta", "sa"), None), P()),
        check_vma=False,
    )
```
